256 devices in a mesh: section: 8 (over x, core), fsdp: 32 (over y, z).
Axes of the slice: x: 4, y: 4, z: 8, core: 2. Of those that a mesh axis runs over, the one named last changes fastest.
Arguments:
- tokens: bfloat16 [8, 2, 4096, 8192], P('section', None, 'fsdp'), may hold values from -6 to 6
- queries: bfloat16 [8, 2, 4096, 4096], P('section', None, 'fsdp'), may hold values from -200 to 200
- gains: bfloat16 [8, 8192], P('section'), may hold values from 0.5 to 1.5
- key_weight: bfloat16 [8, 8192, 512], P('section', 'fsdp'), may hold values from -0.0625 to 0.0625
- value_weight: bfloat16 [8, 8192, 512], P('section', 'fsdp'), may hold values from -0.0625 to 0.0625
- lengths: int32 [2, 64], replicated, may hold values from 1 to 128, 4096 in all within a row
Outputs:
- attended: bfloat16 [8, 2, 4096, 4096], P('section', None, 'fsdp')
The draws below stay inside these ranges and needn't reach their ends.
Inputs may be any that keep to these rules, and one draw needn't show every extreme that they name: `lengths`: each row sums to 4096; some document has exactly 128 tokens.
All inputs are finite; a program needn't handle non-finite values.
Results may differ from the reference program's by a relative error of at most 0.012.
The reference program's roundings to bfloat16 on the way (of `normed`) count: a program that leaves them out, or rounds other values in their place, can miss the bound.
Values may be sent and summed in bfloat16 or wider, within the bound.
A program may use at most 128 MiB of HBM per device.

```python
import math
import jax
import jax.numpy as jnp
import numpy as np
from jax import lax

D = 8192
KV_HEADS = 4
Q_HEADS = 32
HEAD = 128
MICRO = 2
TOK_DEV = 128
TOKENS = 4096
DOCS = 64
LAYERS = 8


def draw_queries(key, part):
    shape = (LAYERS, MICRO, TOKENS, Q_HEADS * HEAD)
    normal_part = jax.random.normal(jax.random.fold_in(key, 11), shape, jnp.float32)
    drawn = jnp.clip(normal_part, -6.0, 6.0)
    return drawn.astype(jnp.bfloat16)


def block_levels(stream_key, extent, pieces, low, high):
    def one(position, blocks):
        draws = jax.random.uniform(jax.random.fold_in(jax.random.fold_in(stream_key, 6), position), (blocks,), jnp.float32, low / len(pieces), high / len(pieces))
        return jnp.repeat(jnp.exp(draws), extent[position] // blocks).reshape((-1,) + (1,) * (len(extent) - position - 1))

    factor_of = one(*pieces[0])
    for cut in pieces[1:]:
        factor_of = factor_of * one(*cut)
    return factor_of


def profile(number_of, total, most, skew):
    portions = [(1 << 20) // math.isqrt(standing ** skew) + 1 for standing in range(2, number_of + 1)]
    spare, holding = total - most - (number_of - 1), [1] * (number_of - 1)
    while spare > 0:
        movable = [i for i in range(number_of - 1) if holding[i] < most]
        mass, remaining = sum([portions[i] for i in movable]), spare
        for i in movable:
            addition = min(most - holding[i], max(1, remaining * portions[i] // mass), spare)
            holding[i] = holding[i] + addition
            spare = spare - addition
    return np.array([most] + holding)


def ragged_sizes(rng, amount, total, most, slope):
    if amount == 2:
        one = jax.random.randint(rng, (), max(1, total - most), min(most, total - 1) + 1)
        return jnp.stack([one, total - one])
    sizes = jnp.asarray(profile(amount, total, most, slope), jnp.int32)
    couples = (amount - 1) // 2
    source_of, taker = sizes[1:1 + 2 * couples:2], sizes[2:2 + 2 * couples:2]
    room = jnp.minimum(source_of - 1, most - taker)
    passed = jax.random.randint(jax.random.fold_in(rng, 1), (couples,), 0, 1 << 20) % (room + 1)
    sizes = sizes.at[1:1 + 2 * couples:2].set(source_of - passed).at[2:2 + 2 * couples:2].set(taker + passed)
    return sizes[jax.random.permutation(jax.random.fold_in(rng, 2), amount)]


def scatter_about(own_key, dims, width, most, pieces=(), kind=jnp.bfloat16):
    values = jax.random.normal(own_key, dims, jnp.float32) * width
    if len(pieces) > 0:
        values = block_levels(own_key, dims, pieces, -0.22, 0.18) * values
    return jnp.clip(values, min=-most, max=most).astype(kind)


def setup_inputs(seed: int = 0) -> dict:
    key_list = jax.random.split(jax.random.key(seed), 7)
    return {
        "tokens": scatter_about(key_list[0], (LAYERS, MICRO, TOKENS, D), 1.0, 6.0, ((0, 8), (2, 32))),
        "queries": draw_queries(jax.random.fold_in(key_list[6], 71), 0),
        "gains": jnp.clip(1.0 + 0.1 * jax.random.normal(key_list[2], (LAYERS, D), jnp.float32), 0.5, 1.5).astype(jnp.bfloat16),
        "key_weight": scatter_about(key_list[3], (LAYERS, D, KV_HEADS * HEAD), D ** -0.5, 0.0625, ((0, 8), (1, 32))),
        "value_weight": scatter_about(key_list[4], (LAYERS, D, KV_HEADS * HEAD), D ** -0.5, 0.0625, ((0, 8), (1, 32))),
        "lengths": jax.vmap(lambda own: ragged_sizes(own, DOCS, TOKENS, TOK_DEV, 2))(jax.random.split(key_list[5], MICRO)).reshape((MICRO, DOCS)).astype(jnp.int32),
    }


def rms_norm(hidden, gain_row):
    widened = hidden.astype(jnp.float32)
    inverse_rms = lax.rsqrt(lax.optimization_barrier(jnp.mean(widened * widened, axis=-1, keepdims=True)) + 1e-05)
    return (widened * inverse_rms * gain_row.astype(jnp.float32)).astype(jnp.bfloat16)

def document_ids(length_row, positions):
    bounds = jnp.cumsum(length_row.astype(jnp.int32))
    return lax.optimization_barrier(jnp.sum((bounds[None, :] <= positions[:, None]).astype(jnp.int32), axis=1))

def block_attend(query_rows, key_rows, value_rows, query_pos, key_pos, query_doc, key_doc):
    query_count = query_rows.shape[0]
    key_count = key_rows.shape[0]
    kv_count = key_rows.shape[1] // HEAD
    group_count = query_rows.shape[1] // (kv_count * HEAD)
    query_heads = query_rows.reshape(query_count, kv_count, group_count, HEAD).astype(jnp.float32)
    key_heads = key_rows.reshape(key_count, kv_count, HEAD).astype(jnp.float32)
    value_heads = value_rows.reshape(key_count, kv_count, HEAD).astype(jnp.float32)
    scores = jnp.einsum('tkgd,skd->kgts', query_heads, key_heads) * HEAD ** (-0.5)
    allowed = (key_doc[None, :] == query_doc[:, None]) & (key_pos[None, :] <= query_pos[:, None]) & (key_pos[None, :] >= 0)
    scores = jnp.where(allowed, scores, -1e+30)
    maxima = lax.optimization_barrier(jnp.max(scores, axis=-1, keepdims=True))
    exponent = jnp.where(allowed, jnp.exp(scores - maxima), 0.0)
    totals = lax.optimization_barrier(jnp.sum(exponent, axis=-1, keepdims=True))
    softmax_rows = (exponent / totals).astype(jnp.bfloat16)
    mixed = jnp.einsum('kgts,skd->tkgd', softmax_rows.astype(jnp.float32), value_heads)
    return mixed.reshape(query_count, kv_count * group_count * HEAD).astype(jnp.bfloat16)

def attend_all(query_all, key_all, value_all, length_row):
    block_count = TOKENS // TOK_DEV
    zero_rows = jnp.zeros((TOK_DEV, key_all.shape[1]), jnp.bfloat16)
    padded_keys = jnp.concatenate([zero_rows, key_all], axis=0)
    padded_values = jnp.concatenate([zero_rows, value_all], axis=0)

    def attend_block(block_index):
        block_start = (block_index * TOK_DEV).astype(jnp.int32)
        query_rows = lax.dynamic_slice_in_dim(query_all, block_start, TOK_DEV, 0)
        key_rows = lax.dynamic_slice_in_dim(padded_keys, block_start, 2 * TOK_DEV, 0)
        value_rows = lax.dynamic_slice_in_dim(padded_values, block_start, 2 * TOK_DEV, 0)
        query_pos = block_start + jnp.arange(TOK_DEV, dtype=jnp.int32)
        key_pos = block_start - TOK_DEV + jnp.arange(2 * TOK_DEV, dtype=jnp.int32)
        return block_attend(query_rows, key_rows, value_rows, query_pos, key_pos, document_ids(length_row, query_pos), document_ids(length_row, key_pos))
    blocks_out = lax.map(attend_block, jnp.arange(block_count, dtype=jnp.int32))
    return blocks_out.reshape(TOKENS, query_all.shape[1])

def reference(tokens, queries, gains, key_weight, value_weight, lengths):
    results = []
    for slot_index in range(MICRO):
        per_layer = []
        for layer_index in range(LAYERS):
            normed = rms_norm(tokens[layer_index, slot_index], gains[layer_index])
            key_all = jnp.dot(normed, key_weight[layer_index], preferred_element_type=jnp.float32).astype(jnp.bfloat16)
            value_all = jnp.dot(normed, value_weight[layer_index], preferred_element_type=jnp.float32).astype(jnp.bfloat16)
            per_layer.append(attend_all(queries[layer_index, slot_index], key_all, value_all, lengths[slot_index]))
        results.append(jnp.stack(per_layer))
    return jnp.stack(results, axis=1)
```

```python
import functools

import jax
import jax.numpy as jnp
from jax import lax
from jax.experimental import pallas as pl
from jax.experimental.pallas import tpu as pltpu
from jax.sharding import PartitionSpec as P

HEAD = 128
GROUPS = 4
FAN = 8
MICRO = 2
TOK = 128
ROWS = 256
BLOCKS = 16
HALF = ROWS * BLOCKS
WIDE = 2 * HEAD
DOCS = 64
XCUT = 4
MESH = pl.DeviceIdType.MESH

FORWARD = ((0, 0), (0, 1), (0, 2), (0, 3), (1, 2))
BACKWARD = ((0, 0), (0, -1), (0, -2), (1, 0), (1, -1))
ACROSS = ((0, 0), (0, 1), (0, 2), (0, -3), (0, 4))


def kernel(
    tok, queries, gains, key_w, value_w, lengths, out,
    wbuf, xown, xoth, xprt, xn, gown, qbuf, obuf, lens, inv_own, inv_send, inv_recv,
    bias, p_own, p_send, p_recv, kv,
    w_send, w_recv, x_send, x_recv, i_send, i_recv, p_ssem, p_rsem, h_send, h_recv, local, o_sem,
):
    me = lax.axis_index("fsdp")
    y, z = me // 8, me % 8
    half, row = y // 2, y % 2
    z_next, z_prev = y * 8 + (z + 1) % 8, y * 8 + (z + 7) % 8
    mate = (y + 1 - 2 * row) * 8 + z
    partner = (3 - y) * 8 + z
    after, before = (me + 1) % 32, (me + 31) % 32

    def block_at(r, d):
        source_row = row if r == 0 else 1 - row
        source_z = (z - d + 8) % 8
        return pl.ds(pl.multiple_of((source_row * 8 + source_z) * ROWS, ROWS), ROWS)

    own_rows = block_at(0, 0)
    own_cols = pl.multiple_of(half * HALF, HALF)
    other_cols = pl.multiple_of((1 - half) * HALF, HALF)

    loads = []
    w_loads = []
    for g in range(GROUPS):
        cols = pl.ds(g * HEAD, HEAD)
        w_loads.append((
            pltpu.make_async_copy(key_w.at[0, :, cols], wbuf.at[g, own_rows, pl.ds(0, HEAD)], local.at[2 * g]),
            pltpu.make_async_copy(value_w.at[0, :, cols], wbuf.at[g, own_rows, pl.ds(HEAD, HEAD)], local.at[2 * g + 1]),
        ))
    for pair in w_loads:
        for c in pair:
            c.start()
    x_other = pltpu.make_async_copy(tok.at[0, :, :, pl.ds(other_cols, HALF)], xoth, local.at[8])
    x_mine = pltpu.make_async_copy(tok.at[0, :, :, pl.ds(own_cols, HALF)], xown, local.at[9])
    g_load = pltpu.make_async_copy(gains.at[:, pl.ds(own_cols, HALF)], gown, local.at[10])
    l_load = pltpu.make_async_copy(lengths, lens, local.at[11])
    q_load = pltpu.make_async_copy(queries.at[0], qbuf, local.at[12])
    for c in (x_other, x_mine, g_load, l_load, q_load):
        c.start()

    barrier = pltpu.get_barrier_semaphore()
    for device in (z_next, z_prev, mate, partner, after, before):
        pl.semaphore_signal(barrier, inc=1, device_id={"fsdp": device}, device_id_type=MESH)
    pl.semaphore_wait(barrier, 6)

    links = ((0, z_next, FORWARD), (1, z_prev, BACKWARD), (2, mate, ACROSS))

    def w_copy(link, g, p, where):
        k, device, _ = links[link]
        return pltpu.make_async_remote_copy(
            src_ref=wbuf.at[g, where],
            dst_ref=wbuf.at[g, where],
            send_sem=w_send.at[k, g, p],
            recv_sem=w_recv.at[k, g, p],
            device_id={"fsdp": device},
            device_id_type=MESH,
        )

    def w_start(g, p):
        for link in (0, 1, 2):
            w_copy(link, g, p, block_at(*links[link][2][p])).start()

    def w_arrive(g, p):
        for link, (dr, dd) in ((0, (0, 1)), (1, (0, -1)), (2, (1, 0))):
            r, d = links[link][2][p]
            w_copy(link, g, p, block_at((r + dr) % 2, d + dd)).wait_recv()

    def w_step(g, p):
        w_arrive(g, p - 1)
        w_start(g, p)

    def x_copy(j):
        width = HALF // XCUT
        return pltpu.make_async_remote_copy(
            src_ref=xoth.at[:, :, pl.ds(j * width, width)],
            dst_ref=xprt.at[:, :, pl.ds(j * width, width)],
            send_sem=x_send.at[j],
            recv_sem=x_recv.at[j],
            device_id={"fsdp": partner},
            device_id_type=MESH,
        )

    def inv_copy():
        return pltpu.make_async_remote_copy(
            src_ref=inv_send, dst_ref=inv_recv, send_sem=i_send, recv_sem=i_recv,
            device_id={"fsdp": partner}, device_id_type=MESH,
        )

    def part_copy(g):
        return pltpu.make_async_remote_copy(
            src_ref=p_send.at[g], dst_ref=p_recv.at[g], send_sem=p_ssem.at[g], recv_sem=p_rsem.at[g],
            device_id={"fsdp": partner}, device_id_type=MESH,
        )

    def halo_copy(g):
        return pltpu.make_async_remote_copy(
            src_ref=kv.at[g, :, pl.ds(TOK, TOK)], dst_ref=kv.at[g, :, pl.ds(0, TOK)],
            send_sem=h_send.at[g], recv_sem=h_recv.at[g],
            device_id={"fsdp": after}, device_id_type=MESH,
        )

    def out_copy(g):
        cols = pl.ds(g * FAN * HEAD, FAN * HEAD)
        return pltpu.make_async_copy(obuf.at[:, :, cols], out.at[0, :, :, cols], o_sem.at[g])

    def eye(n):
        return lax.broadcasted_iota(jnp.int32, (n, n), 0) == lax.broadcasted_iota(jnp.int32, (n, n), 1)

    def squares():
        for m in range(MICRO):
            def add(j, total):
                at = pl.ds(pl.multiple_of(j * 512, 512), 512)
                for x in (xown, xoth):
                    v = x[m, :, at].astype(jnp.float32)
                    v = v * v
                    for i in range(4):
                        total = total + v[:, i * 128:(i + 1) * 128]
                return total
            total = lax.fori_loop(0, HALF // 512, add, jnp.zeros((TOK, 128), jnp.float32))
            mean = jnp.sum(total, axis=1, keepdims=True) * (1.0 / (2 * HALF))
            inverse = jnp.broadcast_to(lax.rsqrt(mean + 1e-05), (TOK, 128))
            inv_own[m] = inverse
            inv_send[m:m + 1, :] = jnp.sum(jnp.where(eye(TOK), inverse, 0.0), axis=0, keepdims=True)

    def normalise(x, base, m, inverse, start, width):
        def one(j, _):
            at = pl.ds(pl.multiple_of(start + j * 256, 256), 256)
            v = x[m, :, at].astype(jnp.float32)
            scaled = v * jnp.concatenate([inverse, inverse], axis=1)
            xn[pl.ds(base + m * TOK, TOK), at] = (scaled * gown[:, at].astype(jnp.float32)).astype(jnp.bfloat16)
            return 0
        lax.fori_loop(0, width // 256, one, 0)

    def normalise_own():
        for m in range(MICRO):
            normalise(xown, 0, m, inv_own[m], 0, HALF)

    def normalise_partner(j):
        for m in range(MICRO):
            line = jnp.broadcast_to(inv_recv[m:m + 1, :], (TOK, TOK))
            column = jnp.sum(jnp.where(eye(TOK), line, 0.0), axis=1, keepdims=True)
            normalise(xprt, 2 * TOK, m, jnp.broadcast_to(column, (TOK, 128)), j * (HALF // XCUT), HALF // XCUT)

    def masks():
        for m in range(MICRO):
            lane = lax.broadcasted_iota(jnp.int32, (DOCS, DOCS), 1)
            sub = lax.broadcasted_iota(jnp.int32, (DOCS, DOCS), 0)
            line = jnp.broadcast_to(lens[m:m + 1, :].astype(jnp.float32), (DOCS, DOCS))
            bound_column = jnp.sum(jnp.where(lane <= sub, line, 0.0), axis=1, keepdims=True)
            column = jnp.sum(jnp.where(lane == sub, line, 0.0), axis=1, keepdims=True)
            bound_line = jnp.sum(jnp.where(sub <= lane, column, 0.0), axis=0, keepdims=True)
            start = me * TOK
            key_pos = (lax.broadcasted_iota(jnp.int32, (DOCS, 2 * TOK), 1) + (start - TOK)).astype(jnp.float32)
            key_doc = jnp.sum(jnp.where(bound_column <= key_pos, 1.0, 0.0), axis=0, keepdims=True)
            query_pos = (lax.broadcasted_iota(jnp.int32, (TOK, DOCS), 0) + start).astype(jnp.float32)
            query_doc = jnp.sum(jnp.where(bound_line <= query_pos, 1.0, 0.0), axis=1, keepdims=True)
            kp = lax.broadcasted_iota(jnp.int32, (TOK, 2 * TOK), 1) + (start - TOK)
            qp = lax.broadcasted_iota(jnp.int32, (TOK, 2 * TOK), 0) + start
            allowed = (key_doc == query_doc) & (kp <= qp) & (kp >= 0)
            bias[m] = jnp.where(allowed, 0.0, -1e30)

    def dot_own(g):
        p_own[g] = jnp.dot(xn[0:2 * TOK, :], wbuf[g], preferred_element_type=jnp.float32)

    def dot_partner(g):
        p_send[g] = jnp.dot(
            xn[2 * TOK:4 * TOK, :], wbuf[g], preferred_element_type=jnp.float32
        ).astype(jnp.bfloat16)

    def finish_kv(g):
        part_copy(g).wait_recv()
        for m in range(MICRO):
            at = pl.ds(m * TOK, TOK)
            kv[g, m, TOK:2 * TOK, :] = (p_own[g, at] + p_recv[g, at].astype(jnp.float32)).astype(jnp.bfloat16)
        halo_copy(g).start()

    def attend(g):
        halo_copy(g).wait_recv()
        factor = HEAD ** (-0.5) * 1.4426950408889634
        for m in range(MICRO):
            keys = kv[g, m, :, 0:HEAD]
            values = kv[g, m, :, HEAD:WIDE]

            def one(j, _):
                at = pl.ds(pl.multiple_of((g * FAN + j) * HEAD, HEAD), HEAD)
                s = lax.dot_general(
                    qbuf[m, :, at], keys, (((1,), (1,)), ((), ())), preferred_element_type=jnp.float32
                ) + bias[m]
                e = jnp.exp2((s - jnp.max(s, axis=1, keepdims=True)) * factor)
                weights = (e * (1.0 / jnp.sum(e, axis=1, keepdims=True))).astype(jnp.bfloat16)
                obuf[m, :, at] = jnp.dot(weights, values, preferred_element_type=jnp.float32).astype(jnp.bfloat16)
                return 0
            lax.fori_loop(0, FAN, one, 0, unroll=True)
        out_copy(g).start()

    for g in (0, 1, 2):
        for c in w_loads[g]:
            c.wait()
        w_start(g, 0)
        if g == 0:
            x_other.wait()
            x_copy(0).start()
    for c in w_loads[3]:
        c.wait()
    x_mine.wait()
    g_load.wait()
    l_load.wait()
    q_load.wait()
    squares()
    inv_copy().start()
    for j in range(1, XCUT):
        x_copy(j).start()
    w_step(0, 1)
    normalise_own()
    w_step(1, 1)
    masks()
    w_step(0, 2)
    w_step(1, 2)
    w_step(0, 3)
    inv_copy().wait_recv()
    x_copy(0).wait_recv()
    normalise_partner(0)
    w_step(1, 3)
    w_step(0, 4)
    w_step(1, 4)
    w_start(3, 0)
    x_copy(1).wait_recv()
    normalise_partner(1)
    w_step(2, 1)
    w_arrive(0, 4)
    dot_own(0)
    w_step(3, 1)
    w_arrive(1, 4)
    dot_own(1)
    w_step(2, 2)
    x_copy(2).wait_recv()
    normalise_partner(2)
    w_step(3, 2)
    w_step(2, 3)
    x_copy(3).wait_recv()
    normalise_partner(3)
    dot_partner(0)
    part_copy(0).start()
    w_step(3, 3)
    dot_partner(1)
    part_copy(1).start()
    w_step(2, 4)
    finish_kv(0)
    w_step(3, 4)
    finish_kv(1)
    w_arrive(2, 4)
    dot_partner(2)
    part_copy(2).start()
    dot_own(2)
    w_arrive(3, 4)
    dot_partner(3)
    part_copy(3).start()
    dot_own(3)
    finish_kv(2)
    attend(0)
    finish_kv(3)
    attend(1)
    attend(2)
    attend(3)

    for g in range(GROUPS):
        for p in range(5):
            for link in (0, 1, 2):
                w_copy(link, g, p, block_at(*links[link][2][p])).wait_send()
    for j in range(XCUT):
        x_copy(j).wait_send()
    inv_copy().wait_send()
    for g in range(GROUPS):
        part_copy(g).wait_send()
        halo_copy(g).wait_send()
        out_copy(g).wait()


def body(tokens, queries, gains, key_weight, value_weight, lengths):
    bf16, f32 = jnp.bfloat16, jnp.float32
    return pl.pallas_call(
        kernel,
        out_shape=jax.ShapeDtypeStruct(queries.shape, bf16),
        in_specs=[pl.BlockSpec(memory_space=pl.ANY)] * 6,
        out_specs=pl.BlockSpec(memory_space=pl.ANY),
        scratch_shapes=[
            pltpu.VMEM((GROUPS, HALF, WIDE), bf16),
            pltpu.VMEM((MICRO, TOK, HALF), bf16),
            pltpu.VMEM((MICRO, TOK, HALF), bf16),
            pltpu.VMEM((MICRO, TOK, HALF), bf16),
            pltpu.VMEM((4 * TOK, HALF), bf16),
            pltpu.VMEM((1, HALF), bf16),
            pltpu.VMEM((MICRO, TOK, GROUPS * FAN * HEAD), bf16),
            pltpu.VMEM((MICRO, TOK, GROUPS * FAN * HEAD), bf16),
            pltpu.VMEM((MICRO, DOCS), jnp.int32),
            pltpu.VMEM((MICRO, TOK, 128), f32),
            pltpu.VMEM((8, 128), f32),
            pltpu.VMEM((8, 128), f32),
            pltpu.VMEM((MICRO, TOK, 2 * TOK), f32),
            pltpu.VMEM((GROUPS, 2 * TOK, WIDE), f32),
            pltpu.VMEM((GROUPS, 2 * TOK, WIDE), bf16),
            pltpu.VMEM((GROUPS, 2 * TOK, WIDE), bf16),
            pltpu.VMEM((GROUPS, MICRO, 2 * TOK, WIDE), bf16),
            pltpu.SemaphoreType.DMA((3, GROUPS, 5)),
            pltpu.SemaphoreType.DMA((3, GROUPS, 5)),
            pltpu.SemaphoreType.DMA((XCUT,)),
            pltpu.SemaphoreType.DMA((XCUT,)),
            pltpu.SemaphoreType.DMA,
            pltpu.SemaphoreType.DMA,
            pltpu.SemaphoreType.DMA((GROUPS,)),
            pltpu.SemaphoreType.DMA((GROUPS,)),
            pltpu.SemaphoreType.DMA((GROUPS,)),
            pltpu.SemaphoreType.DMA((GROUPS,)),
            pltpu.SemaphoreType.DMA((13,)),
            pltpu.SemaphoreType.DMA((GROUPS,)),
        ],
        compiler_params=pltpu.CompilerParams(collective_id=0, has_side_effects=True),
        name="window",
    )(tokens, queries, gains, key_weight, value_weight, lengths)


def solution(mesh):
    return jax.shard_map(
        body,
        mesh=mesh,
        in_specs=(
            P("section", None, "fsdp", None),
            P("section", None, "fsdp", None),
            P("section", None),
            P("section", "fsdp", None),
            P("section", "fsdp", None),
            P(),
        ),
        out_specs=P("section", None, "fsdp", None),
        check_vma=False,
    )
```

```python
import functools

import jax
import jax.numpy as jnp
from jax import lax
from jax.experimental import pallas as pl
from jax.experimental.pallas import tpu as pltpu
from jax.sharding import PartitionSpec as P

HEAD = 128
GROUPS = 4
FAN = 8
MICRO = 2
TOK = 128
ROWS = 256
BLOCKS = 16
HALF = ROWS * BLOCKS
WIDE = 2 * HEAD
DOCS = 64
XCUT = 4
MESH = pl.DeviceIdType.MESH

EVEN = (
    (((0, 0),), ((0, 1),), ((0, 2),), ((0, 3),), ((1, 2),)),
    (((0, 0),), ((0, -1),), ((0, -2),), ((1, 0),), ((1, -1),)),
    (((0, 0),), ((0, 1),), ((0, 2),), ((0, -3),), ((0, 4),)),
)
BACK = (
    (((0, 0),), ((0, 1),), ((0, 2),), ((1, 2),), ()),
    (((0, 0),), ((0, -1),), ((0, -2), (1, 0)), ((0, -3),), ((1, -1),)),
    (((0, 0),), ((0, 1),), ((0, 2),), ((0, -3),), ((0, -4),)),
)
SIDE = (
    (((0, 0),), ((0, 1),), ((0, 2),), ((0, 3),), ()),
    (((0, 0),), ((0, -1),), ((0, -2),), ((1, 0),), ((1, -1),)),
    (((0, 0),), ((0, 1),), ((0, 2),), ((0, 3), (0, -3)), ((0, 4),)),
)
PATTERN = (EVEN, EVEN, BACK, SIDE)
MOVES = ((0, 1), (0, -1), (1, 0))
SENDS = [[[(p, item) for p, items in enumerate(link) for item in items] for link in pattern] for pattern in PATTERN]
ARRIVALS = [
    {
        ((r + MOVES[k][0]) % 2, d + MOVES[k][1]): (k, i)
        for k, link in enumerate(links)
        for i, (_, (r, d)) in enumerate(link)
    }
    for links in SENDS
]
LATE = ((), (), ((1, 3), (1, 4), (2, 4)), ((1, 3), (1, 4), (2, 3), (2, 4)))


def kernel(
    tok, queries, gains, key_w, value_w, lengths, out,
    wbuf, xown, xoth, xprt, xn, gown, qbuf, lens, inv_own, inv_send, inv_recv,
    bias, acc, p_own, p_send, p_recv, kv, passing,
    w_send, w_recv, x_send, x_recv, i_send, i_recv, p_ssem, p_rsem, h_send, h_recv, r_send, r_recv, local,
):
    me = lax.axis_index("fsdp")
    y, z = me // 8, me % 8
    half, row = y // 2, y % 2
    z_next, z_prev = y * 8 + (z + 1) % 8, y * 8 + (z + 7) % 8
    mate = (y + 1 - 2 * row) * 8 + z
    partner = (3 - y) * 8 + z
    below = jnp.minimum(me + 8, 31)
    after, before = (me + 1) % 32, (me + 31) % 32

    def block_at(r, d):
        source_row = row if r == 0 else 1 - row
        source_z = (z - d + 8) % 8
        return pl.ds(pl.multiple_of((source_row * 8 + source_z) * ROWS, ROWS), ROWS)

    own_rows = block_at(0, 0)
    own_cols = pl.multiple_of(half * HALF, HALF)
    other_cols = pl.multiple_of((1 - half) * HALF, HALF)

    loads = []
    w_loads = []
    for g in range(GROUPS):
        cols = pl.ds(g * HEAD, HEAD)
        w_loads.append((
            pltpu.make_async_copy(key_w.at[0, :, cols], wbuf.at[g, own_rows, pl.ds(0, HEAD)], local.at[2 * g]),
            pltpu.make_async_copy(value_w.at[0, :, cols], wbuf.at[g, own_rows, pl.ds(HEAD, HEAD)], local.at[2 * g + 1]),
        ))
    for pair in w_loads:
        for c in pair:
            c.start()
    x_other = pltpu.make_async_copy(tok.at[0, :, :, pl.ds(other_cols, HALF)], xoth, local.at[8])
    x_mine = pltpu.make_async_copy(tok.at[0, :, :, pl.ds(own_cols, HALF)], xown, local.at[9])
    g_load = pltpu.make_async_copy(gains.at[:, pl.ds(own_cols, HALF)], gown, local.at[10])
    l_load = pltpu.make_async_copy(lengths, lens, local.at[11])
    q_load = pltpu.make_async_copy(queries.at[0], qbuf, local.at[12])
    for c in (x_other, x_mine, g_load, l_load, q_load):
        c.start()

    @pl.when(me == 0)
    def _():
        for g in range(GROUPS):
            kv[g, :, 0:TOK, :] = jnp.zeros((MICRO, TOK, WIDE), jnp.bfloat16)

    barrier = pltpu.get_barrier_semaphore()
    for device in (z_next, z_prev, mate, partner, after, before):
        pl.semaphore_signal(barrier, inc=1, device_id={"fsdp": device}, device_id_type=MESH)
    def barrier_wait():
        pl.semaphore_wait(barrier, 6)

    barrier_wait()

    targets = (z_next, z_prev, mate)
    here = [{(0, 0)} for _ in range(GROUPS)]

    def w_copy(g, k, i, where):
        return pltpu.make_async_remote_copy(
            src_ref=wbuf.at[g, where],
            dst_ref=wbuf.at[g, where],
            send_sem=w_send.at[k, g, i],
            recv_sem=w_recv.at[k, g, i],
            device_id={"fsdp": targets[k]},
            device_id_type=MESH,
        )

    def w_need(g, item):
        if item not in here[g]:
            here[g].add(item)
            w_copy(g, *ARRIVALS[g][item], block_at(*item)).wait_recv()

    def w_step(g, p, links=(0, 1, 2), at=None):
        for k in links:
            for i, (position, item) in enumerate(SENDS[g][k]):
                if position == p and at in (None, item):
                    w_need(g, item)
                    w_copy(g, k, i, block_at(*item)).start()

    def w_late(g):
        return [item for item, (k, i) in ARRIVALS[g].items() if (k, SENDS[g][k][i][0]) in LATE[g] and not (
            g == 3 and k == 2 and SENDS[g][k][i][1] == (0, 3))]

    def w_early(g):
        late = w_late(g)
        return [(0, 0)] + [item for item in ARRIVALS[g] if item not in late]

    def w_rest(g, items):
        for item in items:
            w_need(g, item)

    def x_copy(j):
        width = HALF // XCUT
        return pltpu.make_async_remote_copy(
            src_ref=xoth.at[:, :, pl.ds(j * width, width)],
            dst_ref=xprt.at[:, :, pl.ds(j * width, width)],
            send_sem=x_send.at[j],
            recv_sem=x_recv.at[j],
            device_id={"fsdp": partner},
            device_id_type=MESH,
        )

    def inv_copy():
        return pltpu.make_async_remote_copy(
            src_ref=inv_send, dst_ref=inv_recv, send_sem=i_send, recv_sem=i_recv,
            device_id={"fsdp": partner}, device_id_type=MESH,
        )

    def part_copy(g, m):
        at = pl.ds(m * TOK, TOK)
        return pltpu.make_async_remote_copy(
            src_ref=p_send.at[g, at], dst_ref=p_recv.at[g, at],
            send_sem=p_ssem.at[g, m], recv_sem=p_rsem.at[g, m],
            device_id={"fsdp": partner}, device_id_type=MESH,
        )

    def halo_to(g, m, device, into=None):
        return pltpu.make_async_remote_copy(
            src_ref=kv.at[g, m, pl.ds(TOK, TOK)],
            dst_ref=kv.at[g, m, pl.ds(0, TOK)] if into is None else into,
            send_sem=h_send.at[g, m],
            recv_sem=(h_recv.at[g, m] if into is None else r_recv.at[g]),
            device_id={"fsdp": device}, device_id_type=MESH,
        )

    def pass_on(g, m, device):
        return pltpu.make_async_remote_copy(
            src_ref=passing.at[g], dst_ref=kv.at[g, m, pl.ds(0, TOK)],
            send_sem=r_send.at[g], recv_sem=h_recv.at[g, m],
            device_id={"fsdp": device}, device_id_type=MESH,
        )

    def halo_start(g, m):
        @pl.when(z < 7)
        def _():
            halo_to(g, m, z_next).start()

        if g < 2:
            @pl.when((z == 7) & (y < 3))
            def _():
                halo_to(g, m, z_next if m == 1 else below, passing.at[g]).start()
        else:
            @pl.when((z == 7) & (y < 3))
            def _():
                halo_to(g, m, after).start()

    def relay(g):
        if g < 2:
            @pl.when((z == 0) & (y < 3))
            def _():
                halo_to(g, 1, z_next, passing.at[g]).wait_recv()
                pass_on(g, 1, below).start()

            @pl.when((z == 7) & (y > 0))
            def _():
                halo_to(g, 0, z_next, passing.at[g]).wait_recv()
                pass_on(g, 0, z_next).start()

    def eye(n):
        return lax.broadcasted_iota(jnp.int32, (n, n), 0) == lax.broadcasted_iota(jnp.int32, (n, n), 1)

    def squares():
        for m in range(MICRO):
            def add(j, total):
                at = pl.ds(pl.multiple_of(j * 512, 512), 512)
                for x in (xown, xoth):
                    v = x[m, :, at].astype(jnp.float32)
                    v = v * v
                    for i in range(4):
                        total = total + v[:, i * 128:(i + 1) * 128]
                return total
            total = lax.fori_loop(0, HALF // 512, add, jnp.zeros((TOK, 128), jnp.float32))
            mean = jnp.sum(total, axis=1, keepdims=True) * (1.0 / (2 * HALF))
            inverse = jnp.broadcast_to(lax.rsqrt(mean + 1e-05), (TOK, 128))
            inv_own[m] = inverse
            inv_send[m:m + 1, :] = jnp.sum(jnp.where(eye(TOK), inverse, 0.0), axis=0, keepdims=True)

    def normalise(x, base, m, inverse, start, width):
        def one(j, _):
            at = pl.ds(pl.multiple_of(start + j * 256, 256), 256)
            v = x[m, :, at].astype(jnp.float32)
            scaled = v * jnp.concatenate([inverse, inverse], axis=1)
            xn[pl.ds(base + m * TOK, TOK), at] = (scaled * gown[:, at].astype(jnp.float32)).astype(jnp.bfloat16)
            return 0
        lax.fori_loop(0, width // 256, one, 0)

    def normalise_own():
        for m in range(MICRO):
            normalise(xown, 0, m, inv_own[m], 0, HALF)

    def normalise_partner(j):
        for m in range(MICRO):
            line = jnp.broadcast_to(inv_recv[m:m + 1, :], (TOK, TOK))
            column = jnp.sum(jnp.where(eye(TOK), line, 0.0), axis=1, keepdims=True)
            normalise(xprt, 2 * TOK, m, jnp.broadcast_to(column, (TOK, 128)), j * (HALF // XCUT), HALF // XCUT)

    def masks():
        for m in range(MICRO):
            lane = lax.broadcasted_iota(jnp.int32, (DOCS, DOCS), 1)
            sub = lax.broadcasted_iota(jnp.int32, (DOCS, DOCS), 0)
            line = jnp.broadcast_to(lens[m:m + 1, :].astype(jnp.float32), (DOCS, DOCS))
            bound_column = jnp.sum(jnp.where(lane <= sub, line, 0.0), axis=1, keepdims=True)
            column = jnp.sum(jnp.where(lane == sub, line, 0.0), axis=1, keepdims=True)
            bound_line = jnp.sum(jnp.where(sub <= lane, column, 0.0), axis=0, keepdims=True)
            start = me * TOK
            key_pos = (lax.broadcasted_iota(jnp.int32, (DOCS, 2 * TOK), 1) + (start - TOK)).astype(jnp.float32)
            key_doc = jnp.sum(jnp.where(bound_column <= key_pos, 1.0, 0.0), axis=0, keepdims=True)
            query_pos = (lax.broadcasted_iota(jnp.int32, (TOK, DOCS), 0) + start).astype(jnp.float32)
            query_doc = jnp.sum(jnp.where(bound_line <= query_pos, 1.0, 0.0), axis=1, keepdims=True)
            kp = lax.broadcasted_iota(jnp.int32, (TOK, 2 * TOK), 1) + (start - TOK)
            qp = lax.broadcasted_iota(jnp.int32, (TOK, 2 * TOK), 0) + start
            allowed = (key_doc == query_doc) & (kp <= qp) & (kp >= 0)
            bias[m] = jnp.where(allowed, 0.0, -1e30)

    def dot_own(g):
        p_own[g] = jnp.dot(xn[0:2 * TOK, :], wbuf[g], preferred_element_type=jnp.float32)

    def dot_partner(g):
        p_send[g] = jnp.dot(
            xn[2 * TOK:4 * TOK, :], wbuf[g], preferred_element_type=jnp.float32
        ).astype(jnp.bfloat16)
        for m in range(MICRO):
            part_copy(g, m).start()

    def add_blocks(total, g, items, first, count):
        for item in items:
            at = block_at(*item)
            total = total + jnp.dot(
                xn[first:first + count, at], wbuf[g, at, :], preferred_element_type=jnp.float32
            )
        return total

    def dot_early(g):
        for first in (0, 2 * TOK):
            acc[g - 2, first:first + 2 * TOK] = add_blocks(
                jnp.zeros((2 * TOK, WIDE), jnp.float32), g, w_early(g), first, 2 * TOK
            )

    def dot_late(g):
        for m in range(MICRO):
            first = (2 + m) * TOK
            p_send[g, m * TOK:(m + 1) * TOK] = add_blocks(
                acc[g - 2, first:first + TOK], g, w_late(g), first, TOK
            ).astype(jnp.bfloat16)
            part_copy(g, m).start()
        p_own[g] = add_blocks(acc[g - 2, 0:2 * TOK], g, w_late(g), 0, 2 * TOK)

    def part_wait(g, m):
        part_copy(g, m).wait_recv()

    def halo_wait(g, m):
        @pl.when(me > 0)
        def _():
            halo_to(g, m, z_next).wait_recv()

    def x_wait(j):
        x_copy(j).wait_recv()

    def inv_wait():
        inv_copy().wait_recv()

    def start_wait():
        for c in (x_mine, g_load, l_load, q_load):
            c.wait()

    def finish_kv(g, m):
        at = pl.ds(m * TOK, TOK)
        kv[g, m, TOK:2 * TOK, :] = (p_own[g, at] + p_recv[g, at].astype(jnp.float32)).astype(jnp.bfloat16)
        halo_start(g, m)

    def attend(g, m):
        factor = HEAD ** (-0.5) * 1.4426950408889634
        keys = kv[g, m, :, 0:HEAD]
        values = kv[g, m, :, HEAD:WIDE]

        def one(j, _):
            at = pl.ds(pl.multiple_of((g * FAN + j) * HEAD, HEAD), HEAD)
            s = lax.dot_general(
                qbuf[m, :, at], keys, (((1,), (1,)), ((), ())), preferred_element_type=jnp.float32
            ) + bias[m]
            e = jnp.exp2((s - jnp.max(s, axis=1, keepdims=True)) * factor)
            weights = (e * (1.0 / jnp.sum(e, axis=1, keepdims=True))).astype(jnp.bfloat16)
            out[0, m, :, at] = jnp.dot(weights, values, preferred_element_type=jnp.float32).astype(jnp.bfloat16)
            return 0
        lax.fori_loop(0, FAN, one, 0, unroll=True)

    for g in (0, 1, 2):
        for c in w_loads[g]:
            c.wait()
        w_step(g, 0)
        if g == 0:
            x_other.wait()
            x_copy(0).start()
    for c in w_loads[3]:
        c.wait()
    start_wait()
    squares()
    inv_copy().start()
    for j in range(1, XCUT):
        x_copy(j).start()
    w_step(0, 1)
    normalise_own()
    w_step(1, 1)
    masks()
    w_step(0, 2)
    w_step(1, 2)
    w_step(0, 3)
    inv_wait()
    x_wait(0)
    normalise_partner(0)
    w_step(1, 3)
    w_step(0, 4)
    w_step(1, 4)
    w_step(3, 0)
    x_wait(1)
    normalise_partner(1)
    w_step(2, 1)
    w_rest(0, ARRIVALS[0])
    dot_own(0)
    w_rest(1, ARRIVALS[1])
    dot_own(1)
    w_step(3, 1)
    w_step(2, 2)
    x_wait(2)
    normalise_partner(2)
    w_step(3, 2)
    w_step(2, 3)
    x_wait(3)
    normalise_partner(3)
    w_step(3, 3, (0, 2, 1), (0, 3))
    w_step(3, 3, (1,))
    dot_partner(0)
    dot_partner(1)
    w_step(3, 3, (2,), (0, -3))
    w_rest(2, w_early(2))
    dot_early(2)
    for m in range(MICRO):
        part_wait(0, m)
        finish_kv(0, m)
    w_step(2, 4)
    w_step(3, 4, (2,))
    w_rest(3, w_early(3))
    dot_early(3)
    w_step(3, 4, (1,))
    for m in range(MICRO):
        part_wait(1, m)
        finish_kv(1, m)
    relay(0)
    w_rest(2, w_late(2))
    dot_late(2)

    @pl.when((z > 0) | (y == 0))
    def _():
        for m in range(MICRO):
            halo_wait(0, m)
            attend(0, m)

    relay(1)
    w_rest(3, w_late(3))
    dot_late(3)

    @pl.when((z == 0) & (y > 0))
    def _():
        for m in range(MICRO):
            halo_wait(0, m)
            attend(0, m)

    for m in range(MICRO):
        part_wait(2, m)
        finish_kv(2, m)
    part_wait(3, 0)
    finish_kv(3, 0)
    halo_wait(1, 0)
    attend(1, 0)
    relay(2)
    part_wait(3, 1)
    finish_kv(3, 1)
    halo_wait(1, 1)
    attend(1, 1)
    relay(3)
    for g in (2, 3):
        for m in range(MICRO):
            halo_wait(g, m)
            attend(g, m)

    def tail_wait():
        for g in range(GROUPS):
            for k in (0, 1, 2):
                for i, (_, item) in enumerate(SENDS[g][k]):
                    w_copy(g, k, i, block_at(*item)).wait_send()
        for j in range(XCUT):
            x_copy(j).wait_send()
        inv_copy().wait_send()
        for g in range(GROUPS):
            for m in range(MICRO):
                part_copy(g, m).wait_send()

        @pl.when(me < 31)
        def _():
            for g in range(GROUPS):
                for m in range(MICRO):
                    halo_to(g, m, z_next).wait_send()

        @pl.when(((z == 0) & (y < 3)) | ((z == 7) & (y > 0)))
        def _():
            for g in (0, 1):
                pass_on(g, 0, z_next).wait_send()

    tail_wait()


def body(tokens, queries, gains, key_weight, value_weight, lengths):
    bf16, f32 = jnp.bfloat16, jnp.float32
    return pl.pallas_call(
        kernel,
        out_shape=pltpu.VMEM(queries.shape, bf16),
        in_specs=[pl.BlockSpec(memory_space=pl.ANY)] * 6,
        out_specs=pl.BlockSpec(memory_space=pltpu.VMEM),
        scratch_shapes=[
            pltpu.VMEM((GROUPS, HALF, WIDE), bf16),
            pltpu.VMEM((MICRO, TOK, HALF), bf16),
            pltpu.VMEM((MICRO, TOK, HALF), bf16),
            pltpu.VMEM((MICRO, TOK, HALF), bf16),
            pltpu.VMEM((4 * TOK, HALF), bf16),
            pltpu.VMEM((1, HALF), bf16),
            pltpu.VMEM((MICRO, TOK, GROUPS * FAN * HEAD), bf16),
            pltpu.VMEM((MICRO, DOCS), jnp.int32),
            pltpu.VMEM((MICRO, TOK, 128), f32),
            pltpu.VMEM((8, 128), f32),
            pltpu.VMEM((8, 128), f32),
            pltpu.VMEM((MICRO, TOK, 2 * TOK), f32),
            pltpu.VMEM((2, 4 * TOK, WIDE), f32),
            pltpu.VMEM((GROUPS, 2 * TOK, WIDE), f32),
            pltpu.VMEM((GROUPS, 2 * TOK, WIDE), bf16),
            pltpu.VMEM((GROUPS, 2 * TOK, WIDE), bf16),
            pltpu.VMEM((GROUPS, MICRO, 2 * TOK, WIDE), bf16),
            pltpu.VMEM((GROUPS, TOK, WIDE), bf16),
            pltpu.SemaphoreType.DMA((3, GROUPS, 6)),
            pltpu.SemaphoreType.DMA((3, GROUPS, 6)),
            pltpu.SemaphoreType.DMA((XCUT,)),
            pltpu.SemaphoreType.DMA((XCUT,)),
            pltpu.SemaphoreType.DMA,
            pltpu.SemaphoreType.DMA,
            pltpu.SemaphoreType.DMA((GROUPS, MICRO)),
            pltpu.SemaphoreType.DMA((GROUPS, MICRO)),
            pltpu.SemaphoreType.DMA((GROUPS, MICRO)),
            pltpu.SemaphoreType.DMA((GROUPS, MICRO)),
            pltpu.SemaphoreType.DMA((GROUPS,)),
            pltpu.SemaphoreType.DMA((GROUPS,)),
            pltpu.SemaphoreType.DMA((13,)),
        ],
        compiler_params=pltpu.CompilerParams(collective_id=0, has_side_effects=True),
        name="window",
    )(tokens, queries, gains, key_weight, value_weight, lengths)


def solution(mesh):
    return jax.shard_map(
        body,
        mesh=mesh,
        in_specs=(
            P("section", None, "fsdp", None),
            P("section", None, "fsdp", None),
            P("section", None),
            P("section", "fsdp", None),
            P("section", "fsdp", None),
            P(),
        ),
        out_specs=P("section", None, "fsdp", None),
        check_vma=False,
    )
```

```python
import functools

import jax
import jax.numpy as jnp
from jax import lax
from jax.experimental import pallas as pl
from jax.experimental.pallas import tpu as pltpu
from jax.sharding import PartitionSpec as P

HEAD = 128
GROUPS = 4
FAN = 8
MICRO = 2
TOK = 128
ROWS = 256
BLOCKS = 16
HALF = ROWS * BLOCKS
WIDE = 2 * HEAD
DOCS = 64
XCUT = 4
MESH = pl.DeviceIdType.MESH

EVEN = (
    (((0, 0),), ((0, 1),), ((0, 2),), ((0, 3),), ((1, 2),)),
    (((0, 0),), ((0, -1),), ((0, -2),), ((1, 0),), ((1, -1),)),
    (((0, 0),), ((0, 1),), ((0, 2),), ((0, -3),), ((0, 4),)),
)
BACK = (
    (((0, 0),), ((0, 1),), ((0, 2),), ((1, 2),), ()),
    (((0, 0),), ((0, -1),), ((0, -2), (1, 0)), ((0, -3),), ((1, -1),)),
    (((0, 0),), ((0, 1),), ((0, 2),), ((0, -3),), ((0, -4),)),
)
SIDE = (
    (((0, 0),), ((0, 1),), ((0, 2),), ((0, 3),), ()),
    (((0, 0),), ((0, -1),), ((0, -2),), ((1, 0),), ((1, -1),)),
    (((0, 0),), ((0, 1),), ((0, 2),), ((0, 3), (0, -3)), ((0, 4),)),
)
PATTERN = (EVEN, EVEN, BACK, SIDE)
MOVES = ((0, 1), (0, -1), (1, 0))
SENDS = [[[(p, item) for p, items in enumerate(link) for item in items] for link in pattern] for pattern in PATTERN]
ARRIVALS = [
    {
        ((r + MOVES[k][0]) % 2, d + MOVES[k][1]): (k, i)
        for k, link in enumerate(links)
        for i, (_, (r, d)) in enumerate(link)
    }
    for links in SENDS
]
PLACE = {}
for _g, _links in enumerate(SENDS):
    for _k, _link in enumerate(_links):
        for _i in range(len(_link)):
            PLACE[_g, _k, _i] = len(PLACE)
LATE = ((), (), ((1, 3), (1, 4), (2, 4)), ((1, 3), (1, 4), (2, 3), (2, 4)))


def kernel(
    tok, queries, gains, key_w, value_w, lengths, out,
    wbuf, xown, xoth, xprt, xn, gown, qbuf, lens, inv_own, inv_send, inv_recv,
    bias, acc, p_own, p_send, p_recv, kv, passing,
    w_send, w_recv, x_send, x_recv, i_send, i_recv, p_ssem, p_rsem, h_send, h_recv, r_send, r_recv, local,
):
    me = lax.axis_index("fsdp")
    y, z = me // 8, me % 8
    half, row = y // 2, y % 2
    z_next, z_prev = y * 8 + (z + 1) % 8, y * 8 + (z + 7) % 8
    mate = (y + 1 - 2 * row) * 8 + z
    partner = (3 - y) * 8 + z
    below = jnp.minimum(me + 8, 31)
    after, before = (me + 1) % 32, (me + 31) % 32

    def block_at(r, d):
        source_row = row if r == 0 else 1 - row
        source_z = (z - d + 8) % 8
        return pl.ds(pl.multiple_of((source_row * 8 + source_z) * ROWS, ROWS), ROWS)

    own_rows = block_at(0, 0)
    own_cols = pl.multiple_of(half * HALF, HALF)
    other_cols = pl.multiple_of((1 - half) * HALF, HALF)

    loads = []
    w_loads = []
    for g in range(GROUPS):
        cols = pl.ds(g * HEAD, HEAD)
        w_loads.append((
            pltpu.make_async_copy(key_w.at[0, :, cols], wbuf.at[g, own_rows, pl.ds(0, HEAD)], local.at[2 * g]),
            pltpu.make_async_copy(value_w.at[0, :, cols], wbuf.at[g, own_rows, pl.ds(HEAD, HEAD)], local.at[2 * g + 1]),
        ))
    for pair in w_loads:
        for c in pair:
            c.start()
    x_other = pltpu.make_async_copy(tok.at[0, :, :, pl.ds(other_cols, HALF)], xoth, local.at[8])
    x_mine = pltpu.make_async_copy(tok.at[0, :, :, pl.ds(own_cols, HALF)], xown, local.at[9])
    g_load = pltpu.make_async_copy(gains.at[:, pl.ds(own_cols, HALF)], gown, local.at[10])
    l_load = pltpu.make_async_copy(lengths, lens, local.at[11])
    q_load = pltpu.make_async_copy(queries.at[0], qbuf, local.at[12])
    for c in (x_other, x_mine, g_load, l_load, q_load):
        c.start()

    @pl.when(me == 0)
    def _():
        for g in range(GROUPS):
            kv[g, :, 0:TOK, :] = jnp.zeros((MICRO, TOK, WIDE), jnp.bfloat16)

    barrier = pltpu.get_barrier_semaphore()
    for device in (z_next, z_prev, mate, partner, after, before):
        pl.semaphore_signal(barrier, inc=1, device_id={"fsdp": device}, device_id_type=MESH)
    def barrier_wait():
        pl.semaphore_wait(barrier, 6)

    barrier_wait()

    targets = (z_next, z_prev, mate)
    here = [{(0, 0)} for _ in range(GROUPS)]

    def w_copy(g, k, i, where):
        return pltpu.make_async_remote_copy(
            src_ref=wbuf.at[g, where],
            dst_ref=wbuf.at[g, where],
            send_sem=w_send,
            recv_sem=w_recv.at[PLACE[g, k, i]],
            device_id={"fsdp": targets[k]},
            device_id_type=MESH,
        )

    def w_need(g, item):
        if item not in here[g]:
            here[g].add(item)
            w_copy(g, *ARRIVALS[g][item], block_at(*item)).wait_recv()

    def w_step(g, p, links=(0, 1, 2), at=None):
        for k in links:
            for i, (position, item) in enumerate(SENDS[g][k]):
                if position == p and at in (None, item):
                    w_need(g, item)
                    w_copy(g, k, i, block_at(*item)).start()

    def w_late(g):
        return [item for item, (k, i) in ARRIVALS[g].items() if (k, SENDS[g][k][i][0]) in LATE[g] and not (
            g == 3 and k == 2 and SENDS[g][k][i][1] == (0, 3))]

    def w_early(g):
        late = w_late(g)
        return [(0, 0)] + [item for item in ARRIVALS[g] if item not in late]

    def w_rest(g, items):
        for item in items:
            w_need(g, item)

    def x_copy(j):
        width = HALF // XCUT
        return pltpu.make_async_remote_copy(
            src_ref=xoth.at[:, :, pl.ds(j * width, width)],
            dst_ref=xprt.at[:, :, pl.ds(j * width, width)],
            send_sem=x_send.at[j],
            recv_sem=x_recv.at[j],
            device_id={"fsdp": partner},
            device_id_type=MESH,
        )

    def inv_copy():
        return pltpu.make_async_remote_copy(
            src_ref=inv_send, dst_ref=inv_recv, send_sem=i_send, recv_sem=i_recv,
            device_id={"fsdp": partner}, device_id_type=MESH,
        )

    def part_copy(g, m):
        at = pl.ds(m * TOK, TOK)
        return pltpu.make_async_remote_copy(
            src_ref=p_send.at[g, at], dst_ref=p_recv.at[g, at],
            send_sem=p_ssem.at[g, m], recv_sem=p_rsem.at[g, m],
            device_id={"fsdp": partner}, device_id_type=MESH,
        )

    def halo_to(g, m, device, into=None):
        return pltpu.make_async_remote_copy(
            src_ref=kv.at[g, m, pl.ds(TOK, TOK)],
            dst_ref=kv.at[g, m, pl.ds(0, TOK)] if into is None else into,
            send_sem=h_send.at[g, m],
            recv_sem=(h_recv.at[g, m] if into is None else r_recv.at[g]),
            device_id={"fsdp": device}, device_id_type=MESH,
        )

    def pass_on(g, m, device):
        return pltpu.make_async_remote_copy(
            src_ref=passing.at[g], dst_ref=kv.at[g, m, pl.ds(0, TOK)],
            send_sem=r_send.at[g], recv_sem=h_recv.at[g, m],
            device_id={"fsdp": device}, device_id_type=MESH,
        )

    def halo_start(g, m):
        @pl.when(z < 7)
        def _():
            halo_to(g, m, z_next).start()

        if g < 2:
            @pl.when((z == 7) & (y < 3))
            def _():
                halo_to(g, m, z_next if m == 1 else below, passing.at[g]).start()
        else:
            @pl.when((z == 7) & (y < 3))
            def _():
                halo_to(g, m, after).start()

    def relay_first(g):
        @pl.when((z == 0) & (y < 3))
        def _():
            halo_to(g, 1, z_next, passing.at[g]).wait_recv()
            pass_on(g, 1, below).start()

    def relay_last(g):
        @pl.when((z == 7) & (y > 0))
        def _():
            halo_to(g, 0, z_next, passing.at[g]).wait_recv()
            pass_on(g, 0, z_next).start()

    def eye(n):
        return lax.broadcasted_iota(jnp.int32, (n, n), 0) == lax.broadcasted_iota(jnp.int32, (n, n), 1)

    def window():
        return lax.broadcasted_iota(jnp.int32, (TOK, TOK), 1) <= lax.broadcasted_iota(jnp.int32, (TOK, TOK), 0)

    def squares():
        for m in range(MICRO):
            def add(j, total):
                at = pl.ds(pl.multiple_of(j * 512, 512), 512)
                for x in (xown, xoth):
                    v = x[m, :, at].astype(jnp.float32)
                    v = v * v
                    for i in range(4):
                        total = total + v[:, i * 128:(i + 1) * 128]
                return total
            total = lax.fori_loop(0, HALF // 512, add, jnp.zeros((TOK, 128), jnp.float32))
            mean = jnp.sum(total, axis=1, keepdims=True) * (1.0 / (2 * HALF))
            inverse = jnp.broadcast_to(lax.rsqrt(mean + 1e-05), (TOK, 128))
            inv_own[m] = inverse
            inv_send[m:m + 1, :] = jnp.sum(jnp.where(eye(TOK), inverse, 0.0), axis=0, keepdims=True)

    def normalise(x, base, m, inverse, start, width):
        def one(j, _):
            at = pl.ds(pl.multiple_of(start + j * 256, 256), 256)
            v = x[m, :, at].astype(jnp.float32)
            scaled = v * jnp.concatenate([inverse, inverse], axis=1)
            xn[pl.ds(base + m * TOK, TOK), at] = (scaled * gown[:, at].astype(jnp.float32)).astype(jnp.bfloat16)
            return 0
        lax.fori_loop(0, width // 256, one, 0)

    def normalise_own():
        for m in range(MICRO):
            normalise(xown, 0, m, inv_own[m], 0, HALF)

    def normalise_partner(j):
        for m in range(MICRO):
            line = jnp.broadcast_to(inv_recv[m:m + 1, :], (TOK, TOK))
            column = jnp.sum(jnp.where(eye(TOK), line, 0.0), axis=1, keepdims=True)
            normalise(xprt, 2 * TOK, m, jnp.broadcast_to(column, (TOK, 128)), j * (HALF // XCUT), HALF // XCUT)

    def masks():
        for m in range(MICRO):
            lane = lax.broadcasted_iota(jnp.int32, (DOCS, DOCS), 1)
            sub = lax.broadcasted_iota(jnp.int32, (DOCS, DOCS), 0)
            line = jnp.broadcast_to(lens[m:m + 1, :].astype(jnp.float32), (DOCS, DOCS))
            bound_column = jnp.sum(jnp.where(lane <= sub, line, 0.0), axis=1, keepdims=True)
            column = jnp.sum(jnp.where(lane == sub, line, 0.0), axis=1, keepdims=True)
            bound_line = jnp.sum(jnp.where(sub <= lane, column, 0.0), axis=0, keepdims=True)
            start = me * TOK
            key_pos = (lax.broadcasted_iota(jnp.int32, (DOCS, 2 * TOK), 1) + (start - TOK)).astype(jnp.float32)
            key_doc = jnp.sum(jnp.where(bound_column <= key_pos, 1.0, 0.0), axis=0, keepdims=True)
            query_pos = (lax.broadcasted_iota(jnp.int32, (TOK, DOCS), 0) + start).astype(jnp.float32)
            query_doc = jnp.sum(jnp.where(bound_line <= query_pos, 1.0, 0.0), axis=1, keepdims=True)
            kp = lax.broadcasted_iota(jnp.int32, (TOK, 2 * TOK), 1) + (start - TOK)
            qp = lax.broadcasted_iota(jnp.int32, (TOK, 2 * TOK), 0) + start
            allowed = (key_doc == query_doc) & (kp <= qp) & (kp >= 0)
            merged = jnp.where(window(), jnp.where(allowed[:, TOK:], 1.0, 0.0), jnp.where(allowed[:, :TOK], 1.0, 0.0))
            bias[m] = jnp.where(merged > 0.5, 0.0, -1e30)

    def dot_own(g):
        p_own[g] = jnp.dot(xn[0:2 * TOK, :], wbuf[g], preferred_element_type=jnp.float32)

    def dot_partner(g):
        p_send[g] = jnp.dot(
            xn[2 * TOK:4 * TOK, :], wbuf[g], preferred_element_type=jnp.float32
        ).astype(jnp.bfloat16)
        for m in range(MICRO):
            part_copy(g, m).start()

    def add_blocks(total, g, items, first, count):
        for item in items:
            at = block_at(*item)
            total = total + jnp.dot(
                xn[first:first + count, at], wbuf[g, at, :], preferred_element_type=jnp.float32
            )
        return total

    def dot_early(g):
        for first in (0, 2 * TOK):
            acc[g - 2, first:first + 2 * TOK] = add_blocks(
                jnp.zeros((2 * TOK, WIDE), jnp.float32), g, w_early(g), first, 2 * TOK
            )

    def dot_late(g):
        for m in range(MICRO):
            first = (2 + m) * TOK
            p_send[g, m * TOK:(m + 1) * TOK] = add_blocks(
                acc[g - 2, first:first + TOK], g, w_late(g), first, TOK
            ).astype(jnp.bfloat16)
            part_copy(g, m).start()
        p_own[g] = add_blocks(acc[g - 2, 0:2 * TOK], g, w_late(g), 0, 2 * TOK)

    def part_wait(g, m):
        part_copy(g, m).wait_recv()

    def halo_wait(g, m):
        @pl.when(me > 0)
        def _():
            halo_to(g, m, z_next).wait_recv()

    def x_wait(j):
        x_copy(j).wait_recv()

    def inv_wait():
        inv_copy().wait_recv()

    def start_wait():
        for c in (x_mine, g_load, l_load, q_load):
            c.wait()

    def finish_kv(g, m):
        at = pl.ds(m * TOK, TOK)
        kv[g, m, TOK:2 * TOK, :] = (p_own[g, at] + p_recv[g, at].astype(jnp.float32)).astype(jnp.bfloat16)
        halo_start(g, m)

    def attend(g, m):
        factor = HEAD ** (-0.5) * 1.4426950408889634
        keys = kv[g, m, :, 0:HEAD]
        values = jnp.concatenate([kv[g, m, :, HEAD:WIDE], jnp.ones((2 * TOK, HEAD), jnp.bfloat16)], axis=1)
        own = window()
        for j in range(FAN):
            at = pl.ds((g * FAN + j) * HEAD, HEAD)
            s = lax.dot_general(
                qbuf[m, :, at], keys, (((1,), (1,)), ((), ())), preferred_element_type=jnp.float32
            )
            s = jnp.where(own, s[:, TOK:], s[:, :TOK]) + bias[m]
            e = jnp.exp2((s - jnp.max(s, axis=1, keepdims=True)) * factor)
            weights = jnp.concatenate([jnp.where(own, 0.0, e), jnp.where(own, e, 0.0)], axis=1)
            mixed = jnp.dot(weights.astype(jnp.bfloat16), values, preferred_element_type=jnp.float32)
            out[0, m, :, at] = (mixed[:, :HEAD] * (1.0 / mixed[:, HEAD:])).astype(jnp.bfloat16)

    for g in (0, 1, 2):
        for c in w_loads[g]:
            c.wait()
        w_step(g, 0)
        if g == 0:
            x_other.wait()
            x_copy(0).start()
    for c in w_loads[3]:
        c.wait()
    start_wait()
    squares()
    inv_copy().start()
    for j in range(1, XCUT):
        x_copy(j).start()
    w_step(0, 1)
    normalise_own()
    w_step(1, 1)
    masks()
    w_step(0, 2)
    w_step(1, 2)
    w_step(0, 3)
    inv_wait()
    x_wait(0)
    normalise_partner(0)
    w_step(1, 3)
    w_step(0, 4)
    w_step(1, 4)
    w_step(3, 0)
    x_wait(1)
    normalise_partner(1)
    w_step(2, 1)
    w_rest(0, ARRIVALS[0])
    dot_own(0)
    w_rest(1, ARRIVALS[1])
    dot_own(1)
    w_step(3, 1)
    w_step(2, 2)
    x_wait(2)
    normalise_partner(2)
    w_step(3, 2)
    w_step(2, 3)
    x_wait(3)
    normalise_partner(3)
    w_step(3, 3, (0, 2, 1), (0, 3))
    w_step(3, 3, (1,))
    dot_partner(0)
    dot_partner(1)
    w_step(3, 3, (2,), (0, -3))
    w_rest(2, w_early(2))
    dot_early(2)
    for m in range(MICRO):
        part_wait(0, m)
        finish_kv(0, m)
    w_step(2, 4)
    w_step(3, 4, (2,))
    w_rest(3, w_early(3))
    dot_early(3)
    w_step(3, 4, (1,))
    for m in range(MICRO):
        part_wait(1, m)
        finish_kv(1, m)
    relay_first(0)
    relay_last(0)
    w_rest(2, w_late(2))
    dot_late(2)
    edge = (z == 0) & (y > 0)

    @pl.when(jnp.logical_not(edge))
    def _():
        for m in range(MICRO):
            halo_wait(0, m)
            attend(0, m)

    relay_first(1)
    relay_last(1)
    w_rest(3, w_late(3))
    dot_late(3)

    @pl.when(edge)
    def _():
        halo_wait(0, 0)
        attend(0, 0)

    for m in range(MICRO):
        part_wait(2, m)
        finish_kv(2, m)
    part_wait(3, 0)
    finish_kv(3, 0)

    @pl.when(edge)
    def _():
        halo_wait(0, 1)
        attend(0, 1)

    @pl.when(jnp.logical_not(edge))
    def _():
        halo_wait(1, 0)
        attend(1, 0)

    part_wait(3, 1)
    finish_kv(3, 1)

    @pl.when(edge)
    def _():
        halo_wait(1, 0)
        attend(1, 0)

    halo_wait(1, 1)
    attend(1, 1)
    for g in (2, 3):
        for m in range(MICRO):
            halo_wait(g, m)
            attend(g, m)

    def tail_wait():
        sent = wbuf.at[:, pl.ds(0, HALF * len(PLACE) // (GROUPS * BLOCKS))]
        pltpu.make_async_remote_copy(
            src_ref=sent, dst_ref=sent, send_sem=w_send, recv_sem=w_recv.at[0],
            device_id={"fsdp": mate}, device_id_type=MESH,
        ).wait_send()
        for j in range(XCUT):
            x_copy(j).wait_send()
        inv_copy().wait_send()
        for g in range(GROUPS):
            for m in range(MICRO):
                part_copy(g, m).wait_send()

        @pl.when(me < 31)
        def _():
            for g in range(GROUPS):
                for m in range(MICRO):
                    halo_to(g, m, z_next).wait_send()

        @pl.when(((z == 0) & (y < 3)) | ((z == 7) & (y > 0)))
        def _():
            for g in (0, 1):
                pass_on(g, 0, z_next).wait_send()

    tail_wait()


def body(tokens, queries, gains, key_weight, value_weight, lengths):
    bf16, f32 = jnp.bfloat16, jnp.float32
    return pl.pallas_call(
        kernel,
        out_shape=pltpu.VMEM(queries.shape, bf16),
        in_specs=[pl.BlockSpec(memory_space=pl.ANY)] * 6,
        out_specs=pl.BlockSpec(memory_space=pltpu.VMEM),
        scratch_shapes=[
            pltpu.VMEM((GROUPS, HALF, WIDE), bf16),
            pltpu.VMEM((MICRO, TOK, HALF), bf16),
            pltpu.VMEM((MICRO, TOK, HALF), bf16),
            pltpu.VMEM((MICRO, TOK, HALF), bf16),
            pltpu.VMEM((4 * TOK, HALF), bf16),
            pltpu.VMEM((1, HALF), bf16),
            pltpu.VMEM((MICRO, TOK, GROUPS * FAN * HEAD), bf16),
            pltpu.VMEM((MICRO, DOCS), jnp.int32),
            pltpu.VMEM((MICRO, TOK, 128), f32),
            pltpu.VMEM((8, 128), f32),
            pltpu.VMEM((8, 128), f32),
            pltpu.VMEM((MICRO, TOK, TOK), f32),
            pltpu.VMEM((2, 4 * TOK, WIDE), f32),
            pltpu.VMEM((GROUPS, 2 * TOK, WIDE), f32),
            pltpu.VMEM((GROUPS, 2 * TOK, WIDE), bf16),
            pltpu.VMEM((GROUPS, 2 * TOK, WIDE), bf16),
            pltpu.VMEM((GROUPS, MICRO, 2 * TOK, WIDE), bf16),
            pltpu.VMEM((GROUPS, TOK, WIDE), bf16),
            pltpu.SemaphoreType.DMA,
            pltpu.SemaphoreType.DMA((len(PLACE),)),
            pltpu.SemaphoreType.DMA((XCUT,)),
            pltpu.SemaphoreType.DMA((XCUT,)),
            pltpu.SemaphoreType.DMA,
            pltpu.SemaphoreType.DMA,
            pltpu.SemaphoreType.DMA((GROUPS, MICRO)),
            pltpu.SemaphoreType.DMA((GROUPS, MICRO)),
            pltpu.SemaphoreType.DMA((GROUPS, MICRO)),
            pltpu.SemaphoreType.DMA((GROUPS, MICRO)),
            pltpu.SemaphoreType.DMA((GROUPS,)),
            pltpu.SemaphoreType.DMA((GROUPS,)),
            pltpu.SemaphoreType.DMA((13,)),
        ],
        compiler_params=pltpu.CompilerParams(collective_id=0, has_side_effects=True),
        name="window",
    )(tokens, queries, gains, key_weight, value_weight, lengths)


def solution(mesh):
    return jax.shard_map(
        body,
        mesh=mesh,
        in_specs=(
            P("section", None, "fsdp", None),
            P("section", None, "fsdp", None),
            P("section", None),
            P("section", "fsdp", None),
            P("section", "fsdp", None),
            P(),
        ),
        out_specs=P("section", None, "fsdp", None),
        check_vma=False,
    )
```

```python
import functools

import jax
import jax.numpy as jnp
from jax import lax
from jax.experimental import pallas as pl
from jax.experimental.pallas import tpu as pltpu
from jax.sharding import PartitionSpec as P

HEAD = 128
GROUPS = 4
FAN = 8
MICRO = 2
TOK = 128
ROWS = 256
BLOCKS = 16
HALF = ROWS * BLOCKS
WIDE = 2 * HEAD
DOCS = 64
XCUT = 4
MESH = pl.DeviceIdType.MESH

EVEN = (
    (((0, 0),), ((0, 1),), ((0, 2),), ((0, 3),), ((1, 2),)),
    (((0, 0),), ((0, -1),), ((0, -2),), ((1, 0),), ((1, -1),)),
    (((0, 0),), ((0, 1),), ((0, 2),), ((0, -3),), ((0, 4),)),
)
BACK = (
    (((0, 0),), ((0, 1),), ((0, 2),), ((1, 2),), ()),
    (((0, 0),), ((0, -1),), ((0, -2), (1, 0)), ((0, -3),), ((1, -1),)),
    (((0, 0),), ((0, 1),), ((0, 2),), ((0, -3),), ((0, -4),)),
)
SIDE = (
    (((0, 0),), ((0, 1),), ((0, 2),), ((0, 3),), ((1, 3, 1), (1, -3, 1))),
    (((0, 0),), ((0, -1),), ((0, -2),), ((1, 0),), ((1, -1, 0),)),
    (((0, 0),), ((0, 1),), ((0, 2),), ((0, 3), (0, -3)), ((0, 4, 0),)),
)
PATTERN = (EVEN, EVEN, BACK, SIDE)
MOVES = ((0, 1), (0, -1), (1, 0))
SENDS = [[[(p, item) for p, items in enumerate(link) for item in items] for link in pattern] for pattern in PATTERN]
ARRIVALS = [
    {
        ((r + MOVES[k][0]) % 2, d + MOVES[k][1], *part): (k, i)
        for k, link in enumerate(links)
        for i, (_, (r, d, *part)) in enumerate(link)
    }
    for links in SENDS
]
JOINT = {(g, p) for g in range(GROUPS) for p in range(5 if g < 2 else 2)}
PLACE, _semaphores = {}, {}
for _g, _links in enumerate(SENDS):
    for _k, _link in enumerate(_links):
        for _i, (_p, _) in enumerate(_link):
            _name = (_g, _p) if (_g, _p) in JOINT else (_g, _k, _i)
            PLACE[_g, _k, _i] = _semaphores.setdefault(_name, len(_semaphores))
LATE = ((), (), ((0, -4), (1, -2), (1, -4)), ((1, -1), (1, -3), (1, -2), (1, 4)))


def kernel(
    tok, queries, gains, key_w, value_w, lengths, out,
    wbuf, xown, xoth, xprt, xn, gown, qbuf, lens, inv_own, inv_send, inv_recv,
    bias, acc, p_own, p_send, p_recv, kv, passing,
    w_send, w_recv, x_send, x_recv, i_send, i_recv, p_ssem, p_rsem, h_send, h_recv, r_send, r_recv, local,
):
    me = lax.axis_index("fsdp")
    y, z = me // 8, me % 8
    half, row = y // 2, y % 2
    z_next, z_prev = y * 8 + (z + 1) % 8, y * 8 + (z + 7) % 8
    mate = (y + 1 - 2 * row) * 8 + z
    partner = (3 - y) * 8 + z
    below = jnp.minimum(me + 8, 31)
    after, before = (me + 1) % 32, (me + 31) % 32

    def block_at(r, d):
        source_row = row if r == 0 else 1 - row
        source_z = (z - d + 8) % 8
        return pl.ds(pl.multiple_of((source_row * 8 + source_z) * ROWS, ROWS), ROWS)

    own_rows = block_at(0, 0)
    own_cols = pl.multiple_of(half * HALF, HALF)
    other_cols = pl.multiple_of((1 - half) * HALF, HALF)

    loads = []
    w_loads = []
    for g in range(GROUPS):
        cols = pl.ds(g * HEAD, HEAD)
        w_loads.append((
            pltpu.make_async_copy(key_w.at[0, :, cols], wbuf.at[g, own_rows, pl.ds(0, HEAD)], local.at[g]),
            pltpu.make_async_copy(value_w.at[0, :, cols], wbuf.at[g, own_rows, pl.ds(HEAD, HEAD)], local.at[g]),
        ))
    for pair in w_loads:
        for c in pair:
            c.start()
    x_other = pltpu.make_async_copy(tok.at[0, :, :, pl.ds(other_cols, HALF)], xoth, local.at[4])
    x_mine = pltpu.make_async_copy(tok.at[0, :, :, pl.ds(own_cols, HALF)], xown, local.at[5])
    g_load = pltpu.make_async_copy(gains.at[:, pl.ds(own_cols, HALF)], gown, local.at[6])
    l_load = pltpu.make_async_copy(lengths, lens, local.at[7])
    q_load = pltpu.make_async_copy(queries.at[0], qbuf, local.at[8])
    for c in (x_other, x_mine, g_load, l_load, q_load):
        c.start()

    @pl.when(me == 0)
    def _():
        for g in range(GROUPS):
            kv[g, :, 0:TOK, :] = jnp.zeros((MICRO, TOK, WIDE), jnp.bfloat16)

    barrier = pltpu.get_barrier_semaphore()
    for device in (z_next, z_prev, mate, partner, after, before):
        pl.semaphore_signal(barrier, inc=1, device_id={"fsdp": device}, device_id_type=MESH)
    def barrier_wait():
        pl.semaphore_wait(barrier, 6)

    barrier_wait()

    targets = (z_next, z_prev, mate)
    here = [{(0, 0)} for _ in range(GROUPS)]

    def w_ref(g, r, d, *part):
        rows = block_at(r, d)
        return wbuf.at[g, rows, pl.ds(part[0] * HEAD, HEAD)] if part else wbuf.at[g, rows]

    def w_copy(g, k, i, ref):
        return pltpu.make_async_remote_copy(
            src_ref=ref,
            dst_ref=ref,
            send_sem=w_send,
            recv_sem=w_recv.at[PLACE[g, k, i]],
            device_id={"fsdp": targets[k]},
            device_id_type=MESH,
        )

    def w_need(g, item):
        if item in here[g]:
            return
        here[g].add(item)
        if item not in ARRIVALS[g]:
            for half in (0, 1):
                w_need(g, (*item, half))
            return
        k, i = ARRIVALS[g][item]
        p = SENDS[g][k][i][0]
        if (g, p) in JOINT:
            together = {it for it, (kk, ii) in ARRIVALS[g].items() if SENDS[g][kk][ii][0] == p}
            here[g].update(together)
            w_copy(g, k, i, wbuf.at[g, pl.ds(0, len(together) * ROWS)]).wait_recv()
        else:
            w_copy(g, k, i, w_ref(g, *item)).wait_recv()

    def w_step(g, p, links=(0, 1, 2), at=None):
        for k in links:
            for i, (position, item) in enumerate(SENDS[g][k]):
                if position == p and at in (None, item):
                    w_need(g, item[:2])
                    w_copy(g, k, i, w_ref(g, *item)).start()

    def w_late(g):
        return LATE[g]

    def w_early(g):
        return [(0, 0)] + [item for item in ARRIVALS[g] if item[:2] not in LATE[g]]

    def w_rest(g, items):
        for item in items:
            w_need(g, item)

    def w_loaded(g):
        both = wbuf.at[g, own_rows]
        pltpu.make_async_copy(both, both, local.at[g]).wait()

    def x_copy(j):
        width = HALF // XCUT
        return pltpu.make_async_remote_copy(
            src_ref=xoth.at[:, :, pl.ds(j * width, width)],
            dst_ref=xprt.at[:, :, pl.ds(j * width, width)],
            send_sem=x_send,
            recv_sem=x_recv.at[j],
            device_id={"fsdp": partner},
            device_id_type=MESH,
        )

    def inv_copy():
        return pltpu.make_async_remote_copy(
            src_ref=inv_send, dst_ref=inv_recv, send_sem=i_send, recv_sem=i_recv,
            device_id={"fsdp": partner}, device_id_type=MESH,
        )

    def pieces(g):
        return ((0, WIDE),) if g < 3 else ((0, HEAD), (HEAD, HEAD))

    def part_copy(g, m, c):
        first, width = pieces(g)[c]
        at = (g, pl.ds(m * TOK, TOK), pl.ds(first, width))
        return pltpu.make_async_remote_copy(
            src_ref=p_send.at[at], dst_ref=p_recv.at[at],
            send_sem=p_ssem, recv_sem=p_rsem.at[g + c, m],
            device_id={"fsdp": partner}, device_id_type=MESH,
        )

    def halo_to(g, m, device, into=None, c=0):
        first, width = pieces(g)[c]
        return pltpu.make_async_remote_copy(
            src_ref=kv.at[g, m, pl.ds(TOK, TOK), pl.ds(first, width)],
            dst_ref=kv.at[g, m, pl.ds(0, TOK), pl.ds(first, width)] if into is None else into,
            send_sem=h_send,
            recv_sem=(h_recv.at[g + c, m] if into is None else r_recv.at[g]),
            device_id={"fsdp": device}, device_id_type=MESH,
        )

    def pass_on(g, m, device):
        return pltpu.make_async_remote_copy(
            src_ref=passing.at[g], dst_ref=kv.at[g, m, pl.ds(0, TOK)],
            send_sem=r_send, recv_sem=h_recv.at[g, m],
            device_id={"fsdp": device}, device_id_type=MESH,
        )

    def halo_start(g, m, c):
        @pl.when(z < 7)
        def _():
            halo_to(g, m, z_next, c=c).start()

        if g < 2:
            @pl.when((z == 7) & (y < 3))
            def _():
                halo_to(g, m, z_next if m == 1 else below, passing.at[g]).start()
        else:
            @pl.when((z == 7) & ((y == 0) | (y == 2)))
            def _():
                halo_to(g, m, after, c=c).start()

    def halo_last():
        @pl.when((z == 7) & (y == 1))
        def _():
            for g in (2, 3):
                for m in range(MICRO):
                    for c in range(len(pieces(g))):
                        halo_to(g, m, after, c=c).start()

    def relay_first(g):
        @pl.when((z == 0) & (y < 3))
        def _():
            halo_to(g, 1, z_next, passing.at[g]).wait_recv()
            pass_on(g, 1, below).start()

    def relay_last(g):
        @pl.when((z == 7) & (y > 0))
        def _():
            halo_to(g, 0, z_next, passing.at[g]).wait_recv()
            pass_on(g, 0, z_next).start()

    def eye(n):
        return lax.broadcasted_iota(jnp.int32, (n, n), 0) == lax.broadcasted_iota(jnp.int32, (n, n), 1)

    def window():
        return lax.broadcasted_iota(jnp.int32, (TOK, TOK), 1) <= lax.broadcasted_iota(jnp.int32, (TOK, TOK), 0)

    def squares():
        for m in range(MICRO):
            def add(j, total):
                at = pl.ds(pl.multiple_of(j * 512, 512), 512)
                for x in (xown, xoth):
                    v = x[m, :, at].astype(jnp.float32)
                    v = v * v
                    for i in range(4):
                        total = total + v[:, i * 128:(i + 1) * 128]
                return total
            total = lax.fori_loop(0, HALF // 512, add, jnp.zeros((TOK, 128), jnp.float32))
            mean = jnp.sum(total, axis=1, keepdims=True) * (1.0 / (2 * HALF))
            inverse = jnp.broadcast_to(lax.rsqrt(mean + 1e-05), (TOK, 128))
            inv_own[m] = inverse
            inv_send[m:m + 1, :] = jnp.sum(jnp.where(eye(TOK), inverse, 0.0), axis=0, keepdims=True)

    def normalise(x, base, m, inverse, start, width):
        def one(j, _):
            at = pl.ds(pl.multiple_of(start + j * 256, 256), 256)
            v = x[m, :, at].astype(jnp.float32)
            scaled = v * jnp.concatenate([inverse, inverse], axis=1)
            xn[pl.ds(base + m * TOK, TOK), at] = (scaled * gown[:, at].astype(jnp.float32)).astype(jnp.bfloat16)
            return 0
        lax.fori_loop(0, width // 256, one, 0)

    def normalise_own():
        for m in range(MICRO):
            normalise(xown, 0, m, inv_own[m], 0, HALF)

    def normalise_partner(j):
        for m in range(MICRO):
            line = jnp.broadcast_to(inv_recv[m:m + 1, :], (TOK, TOK))
            column = jnp.sum(jnp.where(eye(TOK), line, 0.0), axis=1, keepdims=True)
            normalise(xprt, 2 * TOK, m, jnp.broadcast_to(column, (TOK, 128)), j * (HALF // XCUT), HALF // XCUT)

    def masks():
        for m in range(MICRO):
            lane = lax.broadcasted_iota(jnp.int32, (DOCS, DOCS), 1)
            sub = lax.broadcasted_iota(jnp.int32, (DOCS, DOCS), 0)
            line = jnp.broadcast_to(lens[m:m + 1, :].astype(jnp.float32), (DOCS, DOCS))
            bound_column = jnp.sum(jnp.where(lane <= sub, line, 0.0), axis=1, keepdims=True)
            column = jnp.sum(jnp.where(lane == sub, line, 0.0), axis=1, keepdims=True)
            bound_line = jnp.sum(jnp.where(sub <= lane, column, 0.0), axis=0, keepdims=True)
            start = me * TOK
            key_pos = (lax.broadcasted_iota(jnp.int32, (DOCS, 2 * TOK), 1) + (start - TOK)).astype(jnp.float32)
            key_doc = jnp.sum(jnp.where(bound_column <= key_pos, 1.0, 0.0), axis=0, keepdims=True)
            query_pos = (lax.broadcasted_iota(jnp.int32, (TOK, DOCS), 0) + start).astype(jnp.float32)
            query_doc = jnp.sum(jnp.where(bound_line <= query_pos, 1.0, 0.0), axis=1, keepdims=True)
            kp = lax.broadcasted_iota(jnp.int32, (TOK, 2 * TOK), 1) + (start - TOK)
            qp = lax.broadcasted_iota(jnp.int32, (TOK, 2 * TOK), 0) + start
            allowed = (key_doc == query_doc) & (kp <= qp) & (kp >= 0)
            merged = jnp.where(window(), jnp.where(allowed[:, TOK:], 1.0, 0.0), jnp.where(allowed[:, :TOK], 1.0, 0.0))
            bias[m] = jnp.where(merged > 0.5, 0.0, -1e30)

    def dot_own(g):
        p_own[g] = jnp.dot(xn[0:2 * TOK, :], wbuf[g], preferred_element_type=jnp.float32)

    def dot_partner(g):
        p_send[g] = jnp.dot(
            xn[2 * TOK:4 * TOK, :], wbuf[g], preferred_element_type=jnp.float32
        ).astype(jnp.bfloat16)
        for m in range(MICRO):
            part_copy(g, m, 0).start()

    def add_blocks(total, g, items, first, count):
        for item in items:
            at = block_at(*item)
            total = total + jnp.dot(
                xn[first:first + count, at], wbuf[g, at, :], preferred_element_type=jnp.float32
            )
        return total

    def dot_early(g):
        for first in (0, 2 * TOK):
            acc[g - 2, first:first + 2 * TOK] = add_blocks(
                jnp.zeros((2 * TOK, WIDE), jnp.float32), g, w_early(g), first, 2 * TOK
            )

    def dot_late(g):
        for m in range(MICRO):
            first = (2 + m) * TOK
            p_send[g, m * TOK:(m + 1) * TOK] = add_blocks(
                acc[g - 2, first:first + TOK], g, w_late(g), first, TOK
            ).astype(jnp.bfloat16)
            for c in range(len(pieces(g))):
                part_copy(g, m, c).start()
        p_own[g] = add_blocks(acc[g - 2, 0:2 * TOK], g, w_late(g), 0, 2 * TOK)

    def part_wait(g, m, c=0):
        part_copy(g, m, c).wait_recv()

    def halo_wait(g, m):
        @pl.when(me > 0)
        def _():
            for c in range(len(pieces(g))):
                halo_to(g, m, z_next, c=c).wait_recv()

    def x_wait(j):
        x_copy(j).wait_recv()

    def inv_wait():
        inv_copy().wait_recv()

    def start_wait():
        for c in (x_mine, g_load, l_load, q_load):
            c.wait()

    def finish_kv(g, m):
        at = pl.ds(m * TOK, TOK)
        for c, (first, width) in enumerate(pieces(g)):
            if c > 0:
                part_wait(g, m, c)
            cols = pl.ds(first, width)
            kv[g, m, TOK:2 * TOK, cols] = (p_own[g, at, cols] + p_recv[g, at, cols].astype(jnp.float32)).astype(jnp.bfloat16)
            halo_start(g, m, c)

    def attend(g, m):
        factor = HEAD ** (-0.5) * 1.4426950408889634
        keys = kv[g, m, :, 0:HEAD]
        values = jnp.concatenate([kv[g, m, :, HEAD:WIDE], jnp.ones((2 * TOK, HEAD), jnp.bfloat16)], axis=1)
        own = window()
        for j in range(FAN):
            at = pl.ds((g * FAN + j) * HEAD, HEAD)
            s = lax.dot_general(
                qbuf[m, :, at], keys, (((1,), (1,)), ((), ())), preferred_element_type=jnp.float32
            )
            s = jnp.where(own, s[:, TOK:], s[:, :TOK]) + bias[m]
            e = jnp.exp2((s - jnp.max(s, axis=1, keepdims=True)) * factor)
            weights = jnp.concatenate([jnp.where(own, 0.0, e), jnp.where(own, e, 0.0)], axis=1)
            mixed = jnp.dot(weights.astype(jnp.bfloat16), values, preferred_element_type=jnp.float32)
            out[0, m, :, at] = (mixed[:, :HEAD] * (1.0 / mixed[:, HEAD:])).astype(jnp.bfloat16)

    for g in (0, 1, 2):
        w_loaded(g)
        w_step(g, 0)
        if g == 0:
            x_other.wait()
            x_copy(0).start()
    w_loaded(3)
    start_wait()
    squares()
    inv_copy().start()
    for j in range(1, XCUT):
        x_copy(j).start()
    w_step(0, 1)
    normalise_own()
    w_step(1, 1)
    masks()
    w_step(0, 2)
    w_step(1, 2)
    w_step(0, 3)
    inv_wait()
    x_wait(0)
    normalise_partner(0)
    w_step(1, 3)
    w_step(0, 4)
    w_step(1, 4)
    w_step(3, 0)
    x_wait(1)
    normalise_partner(1)
    w_step(2, 1)
    w_rest(0, ARRIVALS[0])
    dot_own(0)
    w_rest(1, ARRIVALS[1])
    dot_own(1)
    w_step(3, 1)
    w_step(2, 2)
    x_wait(2)
    normalise_partner(2)
    w_step(3, 2)
    w_step(2, 3)
    x_wait(3)
    normalise_partner(3)
    w_step(3, 3, (0, 2, 1), (0, 3))
    w_step(3, 3, (1,))
    dot_partner(0)
    dot_partner(1)
    w_step(3, 3, (2,), (0, -3))
    w_rest(2, w_early(2))
    dot_early(2)
    for m in range(MICRO):
        part_wait(0, m)
        finish_kv(0, m)
    w_step(2, 4)
    w_step(3, 4, (2,))
    w_step(3, 4, (0,), (1, 3, 1))
    w_rest(3, w_early(3))
    dot_early(3)
    w_step(3, 4, (1,))
    w_step(3, 4, (0,), (1, -3, 1))
    for m in range(MICRO):
        part_wait(1, m)
        finish_kv(1, m)
    relay_first(0)
    relay_last(0)
    w_rest(2, w_late(2))
    dot_late(2)
    edge = (z == 0) & (y > 0)

    @pl.when(jnp.logical_not(edge))
    def _():
        for m in range(MICRO):
            halo_wait(0, m)
            attend(0, m)

    w_rest(3, w_late(3))
    dot_late(3)
    relay_first(1)
    relay_last(1)

    @pl.when(edge)
    def _():
        halo_wait(0, 0)
        attend(0, 0)

    for m in range(MICRO):
        part_wait(2, m)
        finish_kv(2, m)
    part_wait(3, 0)
    finish_kv(3, 0)

    @pl.when(edge)
    def _():
        halo_wait(0, 1)
        attend(0, 1)

    @pl.when(jnp.logical_not(edge))
    def _():
        halo_wait(1, 0)
        attend(1, 0)

    part_wait(3, 1)
    finish_kv(3, 1)
    halo_last()
    halo_wait(1, 1)
    attend(1, 1)

    @pl.when(edge)
    def _():
        halo_wait(1, 0)
        attend(1, 0)

    for g in (2, 3):
        for m in range(MICRO):
            halo_wait(g, m)
            attend(g, m)

    def tail_wait():
        sent = wbuf.at[:, pl.ds(0, HALF - ROWS)]
        pltpu.make_async_remote_copy(
            src_ref=sent, dst_ref=sent, send_sem=w_send, recv_sem=w_recv.at[0],
            device_id={"fsdp": mate}, device_id_type=MESH,
        ).wait_send()
        pltpu.make_async_remote_copy(
            src_ref=xoth, dst_ref=xprt, send_sem=x_send, recv_sem=x_recv.at[0],
            device_id={"fsdp": partner}, device_id_type=MESH,
        ).wait_send()
        inv_copy().wait_send()
        pltpu.make_async_remote_copy(
            src_ref=p_send, dst_ref=p_recv, send_sem=p_ssem, recv_sem=p_rsem.at[0, 0],
            device_id={"fsdp": partner}, device_id_type=MESH,
        ).wait_send()

        @pl.when(me < 31)
        def _():
            rows = kv.at[:, :, pl.ds(0, TOK)]
            pltpu.make_async_remote_copy(
                src_ref=rows, dst_ref=rows, send_sem=h_send, recv_sem=h_recv.at[0, 0],
                device_id={"fsdp": z_next}, device_id_type=MESH,
            ).wait_send()

        @pl.when(((z == 0) & (y < 3)) | ((z == 7) & (y > 0)))
        def _():
            pltpu.make_async_remote_copy(
                src_ref=passing, dst_ref=passing, send_sem=r_send, recv_sem=r_recv.at[0],
                device_id={"fsdp": z_next}, device_id_type=MESH,
            ).wait_send()

    tail_wait()


def body(tokens, queries, gains, key_weight, value_weight, lengths):
    bf16, f32 = jnp.bfloat16, jnp.float32
    return pl.pallas_call(
        kernel,
        out_shape=pltpu.VMEM(queries.shape, bf16),
        in_specs=[pl.BlockSpec(memory_space=pl.ANY)] * 6,
        out_specs=pl.BlockSpec(memory_space=pltpu.VMEM),
        scratch_shapes=[
            pltpu.VMEM((GROUPS, HALF, WIDE), bf16),
            pltpu.VMEM((MICRO, TOK, HALF), bf16),
            pltpu.VMEM((MICRO, TOK, HALF), bf16),
            pltpu.VMEM((MICRO, TOK, HALF), bf16),
            pltpu.VMEM((4 * TOK, HALF), bf16),
            pltpu.VMEM((1, HALF), bf16),
            pltpu.VMEM((MICRO, TOK, GROUPS * FAN * HEAD), bf16),
            pltpu.VMEM((MICRO, DOCS), jnp.int32),
            pltpu.VMEM((MICRO, TOK, 128), f32),
            pltpu.VMEM((8, 128), f32),
            pltpu.VMEM((8, 128), f32),
            pltpu.VMEM((MICRO, TOK, TOK), f32),
            pltpu.VMEM((2, 4 * TOK, WIDE), f32),
            pltpu.VMEM((GROUPS, 2 * TOK, WIDE), f32),
            pltpu.VMEM((GROUPS, 2 * TOK, WIDE), bf16),
            pltpu.VMEM((GROUPS, 2 * TOK, WIDE), bf16),
            pltpu.VMEM((GROUPS, MICRO, 2 * TOK, WIDE), bf16),
            pltpu.VMEM((2, TOK, WIDE), bf16),
            pltpu.SemaphoreType.DMA,
            pltpu.SemaphoreType.DMA((len(_semaphores),)),
            pltpu.SemaphoreType.DMA,
            pltpu.SemaphoreType.DMA((XCUT,)),
            pltpu.SemaphoreType.DMA,
            pltpu.SemaphoreType.DMA,
            pltpu.SemaphoreType.DMA,
            pltpu.SemaphoreType.DMA((GROUPS + 1, MICRO)),
            pltpu.SemaphoreType.DMA,
            pltpu.SemaphoreType.DMA((GROUPS + 1, MICRO)),
            pltpu.SemaphoreType.DMA,
            pltpu.SemaphoreType.DMA((2,)),
            pltpu.SemaphoreType.DMA((9,)),
        ],
        compiler_params=pltpu.CompilerParams(collective_id=0, has_side_effects=True),
        name="window",
    )(tokens, queries, gains, key_weight, value_weight, lengths)


def solution(mesh):
    return jax.shard_map(
        body,
        mesh=mesh,
        in_specs=(
            P("section", None, "fsdp", None),
            P("section", None, "fsdp", None),
            P("section", None),
            P("section", "fsdp", None),
            P("section", "fsdp", None),
            P(),
        ),
        out_specs=P("section", None, "fsdp", None),
        check_vma=False,
    )
```

```python
import functools

import jax
import jax.numpy as jnp
from jax import lax
from jax.experimental import pallas as pl
from jax.experimental.pallas import tpu as pltpu
from jax.sharding import PartitionSpec as P

HEAD = 128
GROUPS = 4
FAN = 8
MICRO = 2
TOK = 128
ROWS = 256
BLOCKS = 16
HALF = ROWS * BLOCKS
WIDE = 2 * HEAD
DOCS = 64
XCUT = 4
MESH = pl.DeviceIdType.MESH

EVEN = (
    (((0, 0),), ((0, 1),), ((0, 2),), ((0, 3),), ((1, 2),)),
    (((0, 0),), ((0, -1),), ((0, -2),), ((1, 0),), ((1, -1),)),
    (((0, 0),), ((0, 1),), ((0, 2),), ((0, -3),), ((0, 4),)),
)
BACK = (
    (((0, 0),), ((0, 1),), ((0, 2),), ((1, 2),), ()),
    (((0, 0),), ((0, -1),), ((0, -2), (1, 0)), ((0, -3),), ((1, -1),)),
    (((0, 0),), ((0, 1),), ((0, 2),), ((0, -3),), ((0, -4),)),
)
SIDE = (
    (((0, 0),), ((0, 1),), ((0, 2),), ((0, 3),), ((1, 3, 1), (1, -3, 1))),
    (((0, 0),), ((0, -1),), ((0, -2),), ((1, 0),), ((1, -1, 0),)),
    (((0, 0),), ((0, 1),), ((0, 2),), ((0, 3), (0, -3)), ((0, 4, 0),)),
)
PATTERN = (EVEN, EVEN, BACK, SIDE)
MOVES = ((0, 1), (0, -1), (1, 0))
SENDS = [[[(p, item) for p, items in enumerate(link) for item in items] for link in pattern] for pattern in PATTERN]
ARRIVALS = [
    {
        ((r + MOVES[k][0]) % 2, d + MOVES[k][1], *part): (k, i)
        for k, link in enumerate(links)
        for i, (_, (r, d, *part)) in enumerate(link)
    }
    for links in SENDS
]
JOINT = {(g, p) for g in range(GROUPS) for p in range(5 if g < 2 else 2)}
PLACE, _semaphores = {}, {}
for _g, _links in enumerate(SENDS):
    for _k, _link in enumerate(_links):
        for _i, (_p, _) in enumerate(_link):
            _name = (_g, _p) if (_g, _p) in JOINT else (_g, _k, _i)
            PLACE[_g, _k, _i] = _semaphores.setdefault(_name, len(_semaphores))
LATE = ((), (), ((0, -4), (1, -2), (1, -4)), ((1, -1), (1, -3), (1, -2), (1, 4)))


def kernel(
    tok, queries, gains, key_w, value_w, lengths, out,
    wbuf, xown, xoth, xprt, xn, gown, qbuf, lens, inv_own, inv_send, inv_recv,
    bias, acc, p_own, p_send, p_recv, kv, passing,
    w_send, w_recv, x_send, x_recv, i_send, i_recv, p_ssem, p_rsem, h_send, h_recv, r_send, r_recv, b_send, local,
):
    me = lax.axis_index("fsdp")
    y, z = me // 8, me % 8
    half, row = y // 2, y % 2
    second = lax.axis_index("section") % 2 == 1
    z_next, z_prev = y * 8 + (z + 1) % 8, y * 8 + (z + 7) % 8
    mate = (y + 1 - 2 * row) * 8 + z
    partner = (3 - y) * 8 + z
    below = jnp.minimum(me + 8, 31)
    after, before = (me + 1) % 32, (me + 31) % 32

    def block_at(r, d):
        source_row = row if r == 0 else 1 - row
        source_z = (z - d + 8) % 8
        return pl.ds(pl.multiple_of((source_row * 8 + source_z) * ROWS, ROWS), ROWS)

    own_rows = block_at(0, 0)
    own_cols = pl.multiple_of(half * HALF, HALF)
    other_cols = pl.multiple_of((1 - half) * HALF, HALF)

    loads = []
    w_loads = []
    for g in range(GROUPS):
        cols = pl.ds(g * HEAD, HEAD)
        w_loads.append((
            pltpu.make_async_copy(key_w.at[0, :, cols], wbuf.at[g, own_rows, pl.ds(0, HEAD)], local.at[g]),
            pltpu.make_async_copy(value_w.at[0, :, cols], wbuf.at[g, own_rows, pl.ds(HEAD, HEAD)], local.at[g]),
        ))
    for pair in w_loads:
        for c in pair:
            c.start()
    x_other = pltpu.make_async_copy(tok.at[0, :, :, pl.ds(other_cols, HALF)], xoth, local.at[4])
    x_mine = pltpu.make_async_copy(tok.at[0, :, :, pl.ds(own_cols, HALF)], xown, local.at[5])
    g_load = pltpu.make_async_copy(gains.at[:, pl.ds(own_cols, HALF)], gown, local.at[6])
    l_load = pltpu.make_async_copy(lengths, lens, local.at[7])
    q_load = pltpu.make_async_copy(queries.at[0], qbuf, local.at[8])
    for c in (x_other, x_mine, g_load, l_load, q_load):
        c.start()

    @pl.when(me == 0)
    def _():
        for g in range(GROUPS):
            kv[g, :, 0:TOK, :] = jnp.zeros((MICRO, TOK, WIDE), jnp.bfloat16)

    barrier = pltpu.get_barrier_semaphore()
    for device in (z_next, z_prev, mate, partner, after, before):
        pl.semaphore_signal(barrier, inc=1, device_id={"fsdp": device}, device_id_type=MESH)
    def barrier_wait():
        pl.semaphore_wait(barrier, 6)

    barrier_wait()

    targets = (z_next, z_prev, mate)
    here = [{(0, 0)} for _ in range(GROUPS)]

    def w_ref(g, r, d, *part):
        rows = block_at(r, d)
        return wbuf.at[g, rows, pl.ds(part[0] * HEAD, HEAD)] if part else wbuf.at[g, rows]

    def w_copy(g, k, i, ref):
        return pltpu.make_async_remote_copy(
            src_ref=ref,
            dst_ref=ref,
            send_sem=w_send,
            recv_sem=w_recv.at[PLACE[g, k, i]],
            device_id={"fsdp": targets[k]},
            device_id_type=MESH,
        )

    def w_need(g, item):
        if item in here[g]:
            return
        here[g].add(item)
        if item not in ARRIVALS[g]:
            for half in (0, 1):
                w_need(g, (*item, half))
            return
        k, i = ARRIVALS[g][item]
        p = SENDS[g][k][i][0]
        if (g, p) in JOINT:
            together = {it for it, (kk, ii) in ARRIVALS[g].items() if SENDS[g][kk][ii][0] == p}
            here[g].update(together)
            w_copy(g, k, i, wbuf.at[g, pl.ds(0, len(together) * ROWS)]).wait_recv()
        else:
            w_copy(g, k, i, w_ref(g, *item)).wait_recv()

    def w_step(g, p, links=(0, 1, 2), at=None):
        for k in links:
            for i, (position, item) in enumerate(SENDS[g][k]):
                if position == p and at in (None, item):
                    w_need(g, item[:2])
                    w_copy(g, k, i, w_ref(g, *item)).start()

    def w_late(g):
        return LATE[g]

    def w_early(g):
        return [(0, 0)] + [item for item in ARRIVALS[g] if item[:2] not in LATE[g]]

    def w_rest(g, items):
        for item in items:
            w_need(g, item)

    def w_loaded(g):
        both = wbuf.at[g, own_rows]
        pltpu.make_async_copy(both, both, local.at[g]).wait()

    def x_copy(j):
        width = HALF // XCUT
        return pltpu.make_async_remote_copy(
            src_ref=xoth.at[:, :, pl.ds(j * width, width)],
            dst_ref=xprt.at[:, :, pl.ds(j * width, width)],
            send_sem=x_send,
            recv_sem=x_recv.at[j],
            device_id={"fsdp": partner},
            device_id_type=MESH,
        )

    def inv_copy():
        return pltpu.make_async_remote_copy(
            src_ref=inv_send, dst_ref=inv_recv, send_sem=i_send, recv_sem=i_recv,
            device_id={"fsdp": partner}, device_id_type=MESH,
        )

    def pieces(g):
        return ((0, WIDE),) if g < 3 else ((0, HEAD), (HEAD, HEAD))

    def part_copy(g, m, c):
        first, width = pieces(g)[c]
        at = (g, pl.ds(m * TOK, TOK), pl.ds(first, width))
        return pltpu.make_async_remote_copy(
            src_ref=p_send.at[at], dst_ref=p_recv.at[at],
            send_sem=p_ssem, recv_sem=p_rsem.at[g + c, m],
            device_id={"fsdp": partner}, device_id_type=MESH,
        )

    def halo_to(g, m, device, into=None, slot=0, c=0):
        first, width = pieces(g)[c]
        return pltpu.make_async_remote_copy(
            src_ref=kv.at[g, m, pl.ds(TOK, TOK), pl.ds(first, width)],
            dst_ref=kv.at[g, m, pl.ds(0, TOK), pl.ds(first, width)] if into is None else into,
            send_sem=h_send,
            recv_sem=(h_recv.at[g + c, m] if into is None else r_recv.at[g + slot]),
            device_id={"fsdp": device}, device_id_type=MESH,
        )

    def pass_on(g, m, device):
        return pltpu.make_async_remote_copy(
            src_ref=passing.at[g], dst_ref=kv.at[g, m, pl.ds(0, TOK)],
            send_sem=r_send, recv_sem=h_recv.at[g, m],
            device_id={"fsdp": device}, device_id_type=MESH,
        )

    def halo_start(g, m, c):
        @pl.when(z < 7)
        def _():
            halo_to(g, m, z_next, c=c).start()

        if g < 2:
            @pl.when((z == 7) & (y < 3))
            def _():
                halo_to(g, m, z_next if m == 1 else below, passing.at[g]).start()
        else:
            @pl.when((z == 7) & ((y == 0) | (y == 2)))
            def _():
                halo_to(g, m, after, c=c).start()

            if g == 2:
                @pl.when((z == 7) & (y == 1) & second)
                def _():
                    halo_to(g, m, below, passing.at[2 + m], m).start()

    def halo_last():
        for groups, turn in (((2, 3), jnp.logical_not(second)), ((3,), second)):
            @pl.when((z == 7) & (y == 1) & turn)
            def _():
                for g in groups:
                    for m in range(MICRO):
                        for c in range(len(pieces(g))):
                            halo_to(g, m, after, c=c).start()

    def pass_round(m):
        return pltpu.make_async_remote_copy(
            src_ref=passing.at[2 + m], dst_ref=kv.at[2, m, pl.ds(0, TOK)],
            send_sem=b_send, recv_sem=h_recv.at[2, m],
            device_id={"fsdp": z_next}, device_id_type=MESH,
        )

    def relay_round():
        @pl.when((z == 7) & (y == 2) & second)
        def _():
            for m in range(MICRO):
                halo_to(2, m, z_next, passing.at[2 + m], m).wait_recv()
                pass_round(m).start()

    def relay_first(g):
        @pl.when((z == 0) & (y < 3))
        def _():
            halo_to(g, 1, z_next, passing.at[g]).wait_recv()
            pass_on(g, 1, below).start()

    def relay_last(g):
        @pl.when((z == 7) & (y > 0))
        def _():
            halo_to(g, 0, z_next, passing.at[g]).wait_recv()
            pass_on(g, 0, z_next).start()

    def eye(n):
        return lax.broadcasted_iota(jnp.int32, (n, n), 0) == lax.broadcasted_iota(jnp.int32, (n, n), 1)

    def window():
        return lax.broadcasted_iota(jnp.int32, (TOK, TOK), 1) <= lax.broadcasted_iota(jnp.int32, (TOK, TOK), 0)

    def squares():
        for m in range(MICRO):
            def add(j, total):
                at = pl.ds(pl.multiple_of(j * 512, 512), 512)
                for x in (xown, xoth):
                    v = x[m, :, at].astype(jnp.float32)
                    v = v * v
                    for i in range(4):
                        total = total + v[:, i * 128:(i + 1) * 128]
                return total
            total = lax.fori_loop(0, HALF // 512, add, jnp.zeros((TOK, 128), jnp.float32))
            mean = jnp.sum(total, axis=1, keepdims=True) * (1.0 / (2 * HALF))
            inverse = jnp.broadcast_to(lax.rsqrt(mean + 1e-05), (TOK, 128))
            inv_own[m] = inverse
            inv_send[m:m + 1, :] = jnp.sum(jnp.where(eye(TOK), inverse, 0.0), axis=0, keepdims=True)

    def normalise(x, base, m, inverse, start, width):
        def one(j, _):
            at = pl.ds(pl.multiple_of(start + j * 256, 256), 256)
            v = x[m, :, at].astype(jnp.float32)
            scaled = v * jnp.concatenate([inverse, inverse], axis=1)
            xn[pl.ds(base + m * TOK, TOK), at] = (scaled * gown[:, at].astype(jnp.float32)).astype(jnp.bfloat16)
            return 0
        lax.fori_loop(0, width // 256, one, 0)

    def normalise_own():
        for m in range(MICRO):
            normalise(xown, 0, m, inv_own[m], 0, HALF)

    def normalise_partner(j):
        for m in range(MICRO):
            line = jnp.broadcast_to(inv_recv[m:m + 1, :], (TOK, TOK))
            column = jnp.sum(jnp.where(eye(TOK), line, 0.0), axis=1, keepdims=True)
            normalise(xprt, 2 * TOK, m, jnp.broadcast_to(column, (TOK, 128)), j * (HALF // XCUT), HALF // XCUT)

    def masks():
        for m in range(MICRO):
            lane = lax.broadcasted_iota(jnp.int32, (DOCS, DOCS), 1)
            sub = lax.broadcasted_iota(jnp.int32, (DOCS, DOCS), 0)
            line = jnp.broadcast_to(lens[m:m + 1, :].astype(jnp.float32), (DOCS, DOCS))
            bound_column = jnp.sum(jnp.where(lane <= sub, line, 0.0), axis=1, keepdims=True)
            column = jnp.sum(jnp.where(lane == sub, line, 0.0), axis=1, keepdims=True)
            bound_line = jnp.sum(jnp.where(sub <= lane, column, 0.0), axis=0, keepdims=True)
            start = me * TOK
            key_pos = (lax.broadcasted_iota(jnp.int32, (DOCS, 2 * TOK), 1) + (start - TOK)).astype(jnp.float32)
            key_doc = jnp.sum(jnp.where(bound_column <= key_pos, 1.0, 0.0), axis=0, keepdims=True)
            query_pos = (lax.broadcasted_iota(jnp.int32, (TOK, DOCS), 0) + start).astype(jnp.float32)
            query_doc = jnp.sum(jnp.where(bound_line <= query_pos, 1.0, 0.0), axis=1, keepdims=True)
            kp = lax.broadcasted_iota(jnp.int32, (TOK, 2 * TOK), 1) + (start - TOK)
            qp = lax.broadcasted_iota(jnp.int32, (TOK, 2 * TOK), 0) + start
            allowed = (key_doc == query_doc) & (kp <= qp) & (kp >= 0)
            merged = jnp.where(window(), jnp.where(allowed[:, TOK:], 1.0, 0.0), jnp.where(allowed[:, :TOK], 1.0, 0.0))
            bias[m] = jnp.where(merged > 0.5, 0.0, -1e30)

    def dot_own(g):
        p_own[g] = jnp.dot(xn[0:2 * TOK, :], wbuf[g], preferred_element_type=jnp.float32)

    def dot_partner(g):
        p_send[g] = jnp.dot(
            xn[2 * TOK:4 * TOK, :], wbuf[g], preferred_element_type=jnp.float32
        ).astype(jnp.bfloat16)
        for m in range(MICRO):
            part_copy(g, m, 0).start()

    def add_blocks(total, g, items, first, count):
        for item in items:
            at = block_at(*item)
            total = total + jnp.dot(
                xn[first:first + count, at], wbuf[g, at, :], preferred_element_type=jnp.float32
            )
        return total

    def dot_early(g):
        for first in (0, 2 * TOK):
            acc[g - 2, first:first + 2 * TOK] = add_blocks(
                jnp.zeros((2 * TOK, WIDE), jnp.float32), g, w_early(g), first, 2 * TOK
            )

    def dot_late(g):
        for m in range(MICRO):
            first = (2 + m) * TOK
            p_send[g, m * TOK:(m + 1) * TOK] = add_blocks(
                acc[g - 2, first:first + TOK], g, w_late(g), first, TOK
            ).astype(jnp.bfloat16)
            for c in range(len(pieces(g))):
                part_copy(g, m, c).start()
        p_own[g] = add_blocks(acc[g - 2, 0:2 * TOK], g, w_late(g), 0, 2 * TOK)

    def part_wait(g, m, c=0):
        part_copy(g, m, c).wait_recv()

    def halo_wait(g, m):
        @pl.when(me > 0)
        def _():
            for c in range(len(pieces(g))):
                halo_to(g, m, z_next, c=c).wait_recv()

    def x_wait(j):
        x_copy(j).wait_recv()

    def inv_wait():
        inv_copy().wait_recv()

    def start_wait():
        for c in (x_mine, g_load, l_load, q_load):
            c.wait()

    def finish_kv(g, m):
        at = pl.ds(m * TOK, TOK)
        for c, (first, width) in enumerate(pieces(g)):
            if c > 0:
                part_wait(g, m, c)
            cols = pl.ds(first, width)
            kv[g, m, TOK:2 * TOK, cols] = (p_own[g, at, cols] + p_recv[g, at, cols].astype(jnp.float32)).astype(jnp.bfloat16)
            halo_start(g, m, c)

    def attend(g, m):
        factor = HEAD ** (-0.5) * 1.4426950408889634
        keys = kv[g, m, :, 0:HEAD]
        values = jnp.concatenate([kv[g, m, :, HEAD:WIDE], jnp.ones((2 * TOK, HEAD), jnp.bfloat16)], axis=1)
        own = window()
        for j in range(FAN):
            at = pl.ds((g * FAN + j) * HEAD, HEAD)
            s = lax.dot_general(
                qbuf[m, :, at], keys, (((1,), (1,)), ((), ())), preferred_element_type=jnp.float32
            )
            s = jnp.where(own, s[:, TOK:], s[:, :TOK]) + bias[m]
            e = jnp.exp2((s - jnp.max(s, axis=1, keepdims=True)) * factor)
            weights = jnp.concatenate([jnp.where(own, 0.0, e), jnp.where(own, e, 0.0)], axis=1)
            mixed = jnp.dot(weights.astype(jnp.bfloat16), values, preferred_element_type=jnp.float32)
            out[0, m, :, at] = (mixed[:, :HEAD] * (1.0 / mixed[:, HEAD:])).astype(jnp.bfloat16)

    for g in (0, 1, 2):
        w_loaded(g)
        w_step(g, 0)
        if g == 0:
            x_other.wait()
            x_copy(0).start()
    w_loaded(3)
    start_wait()
    squares()
    inv_copy().start()
    for j in range(1, XCUT):
        x_copy(j).start()
    w_step(0, 1)
    normalise_own()
    w_step(1, 1)
    masks()
    w_step(0, 2)
    w_step(1, 2)
    w_step(0, 3)
    inv_wait()
    x_wait(0)
    normalise_partner(0)
    w_step(1, 3)
    w_step(0, 4)
    w_step(1, 4)
    w_step(3, 0)
    x_wait(1)
    normalise_partner(1)
    w_step(2, 1)
    w_rest(0, ARRIVALS[0])
    dot_own(0)
    w_rest(1, ARRIVALS[1])
    dot_own(1)
    w_step(3, 1)
    w_step(2, 2)
    x_wait(2)
    normalise_partner(2)
    w_step(3, 2)
    w_step(2, 3)
    x_wait(3)
    normalise_partner(3)
    w_step(3, 3, (0, 2, 1), (0, 3))
    w_step(3, 3, (1,))
    dot_partner(0)
    dot_partner(1)
    w_step(3, 3, (2,), (0, -3))
    w_rest(2, w_early(2))
    dot_early(2)
    for m in range(MICRO):
        part_wait(0, m)
        finish_kv(0, m)
    w_step(2, 4)
    w_step(3, 4, (2,))
    w_step(3, 4, (0,), (1, 3, 1))
    w_rest(3, w_early(3))
    dot_early(3)
    w_step(3, 4, (1,))
    w_step(3, 4, (0,), (1, -3, 1))
    for m in range(MICRO):
        part_wait(1, m)
        finish_kv(1, m)
    relay_first(0)
    relay_last(0)
    w_rest(2, w_late(2))
    dot_late(2)
    edge = (z == 0) & (y > 0)

    @pl.when(jnp.logical_not(edge) & (z < 7))
    def _():
        for m in range(MICRO):
            halo_wait(0, m)
            attend(0, m)

    w_rest(3, w_late(3))
    dot_late(3)
    relay_first(1)
    relay_last(1)

    @pl.when(edge)
    def _():
        halo_wait(0, 0)
        attend(0, 0)

    for m in range(MICRO):
        part_wait(2, m)
        finish_kv(2, m)
    part_wait(3, 0)
    finish_kv(3, 0)

    @pl.when(edge)
    def _():
        halo_wait(0, 1)
        attend(0, 1)

    @pl.when(jnp.logical_not(edge))
    def _():
        halo_wait(1, 0)
        attend(1, 0)

    part_wait(3, 1)
    finish_kv(3, 1)
    @pl.when(z == 7)
    def _():
        for m in range(MICRO):
            halo_wait(0, m)
            attend(0, m)

    halo_last()

    halo_wait(1, 1)
    attend(1, 1)
    relay_round()

    @pl.when(edge)
    def _():
        halo_wait(1, 0)
        attend(1, 0)

    for g in (2, 3):
        for m in range(MICRO):
            halo_wait(g, m)
            attend(g, m)

    def tail_wait():
        sent = wbuf.at[:, pl.ds(0, HALF - ROWS)]
        pltpu.make_async_remote_copy(
            src_ref=sent, dst_ref=sent, send_sem=w_send, recv_sem=w_recv.at[0],
            device_id={"fsdp": mate}, device_id_type=MESH,
        ).wait_send()
        pltpu.make_async_remote_copy(
            src_ref=xoth, dst_ref=xprt, send_sem=x_send, recv_sem=x_recv.at[0],
            device_id={"fsdp": partner}, device_id_type=MESH,
        ).wait_send()
        inv_copy().wait_send()
        pltpu.make_async_remote_copy(
            src_ref=p_send, dst_ref=p_recv, send_sem=p_ssem, recv_sem=p_rsem.at[0, 0],
            device_id={"fsdp": partner}, device_id_type=MESH,
        ).wait_send()

        @pl.when(me < 31)
        def _():
            rows = kv.at[:, :, pl.ds(0, TOK)]
            pltpu.make_async_remote_copy(
                src_ref=rows, dst_ref=rows, send_sem=h_send, recv_sem=h_recv.at[0, 0],
                device_id={"fsdp": z_next}, device_id_type=MESH,
            ).wait_send()

        @pl.when(((z == 0) & (y < 3)) | ((z == 7) & (y > 0)))
        def _():
            pltpu.make_async_remote_copy(
                src_ref=passing.at[pl.ds(0, 2)], dst_ref=passing.at[pl.ds(0, 2)], send_sem=r_send, recv_sem=r_recv.at[0],
                device_id={"fsdp": z_next}, device_id_type=MESH,
            ).wait_send()

        @pl.when((z == 7) & (y == 2) & second)
        def _():
            both = passing.at[pl.ds(2, 2)]
            pltpu.make_async_remote_copy(
                src_ref=both, dst_ref=both, send_sem=b_send, recv_sem=r_recv.at[2],
                device_id={"fsdp": z_next}, device_id_type=MESH,
            ).wait_send()

    tail_wait()


def body(tokens, queries, gains, key_weight, value_weight, lengths):
    bf16, f32 = jnp.bfloat16, jnp.float32
    return pl.pallas_call(
        kernel,
        out_shape=pltpu.VMEM(queries.shape, bf16),
        in_specs=[pl.BlockSpec(memory_space=pl.ANY)] * 6,
        out_specs=pl.BlockSpec(memory_space=pltpu.VMEM),
        scratch_shapes=[
            pltpu.VMEM((GROUPS, HALF, WIDE), bf16),
            pltpu.VMEM((MICRO, TOK, HALF), bf16),
            pltpu.VMEM((MICRO, TOK, HALF), bf16),
            pltpu.VMEM((MICRO, TOK, HALF), bf16),
            pltpu.VMEM((4 * TOK, HALF), bf16),
            pltpu.VMEM((1, HALF), bf16),
            pltpu.VMEM((MICRO, TOK, GROUPS * FAN * HEAD), bf16),
            pltpu.VMEM((MICRO, DOCS), jnp.int32),
            pltpu.VMEM((MICRO, TOK, 128), f32),
            pltpu.VMEM((8, 128), f32),
            pltpu.VMEM((8, 128), f32),
            pltpu.VMEM((MICRO, TOK, TOK), f32),
            pltpu.VMEM((2, 4 * TOK, WIDE), f32),
            pltpu.VMEM((GROUPS, 2 * TOK, WIDE), f32),
            pltpu.VMEM((GROUPS, 2 * TOK, WIDE), bf16),
            pltpu.VMEM((GROUPS, 2 * TOK, WIDE), bf16),
            pltpu.VMEM((GROUPS, MICRO, 2 * TOK, WIDE), bf16),
            pltpu.VMEM((4, TOK, WIDE), bf16),
            pltpu.SemaphoreType.DMA,
            pltpu.SemaphoreType.DMA((len(_semaphores),)),
            pltpu.SemaphoreType.DMA,
            pltpu.SemaphoreType.DMA((XCUT,)),
            pltpu.SemaphoreType.DMA,
            pltpu.SemaphoreType.DMA,
            pltpu.SemaphoreType.DMA,
            pltpu.SemaphoreType.DMA((GROUPS + 1, MICRO)),
            pltpu.SemaphoreType.DMA,
            pltpu.SemaphoreType.DMA((GROUPS + 1, MICRO)),
            pltpu.SemaphoreType.DMA,
            pltpu.SemaphoreType.DMA((4,)),
            pltpu.SemaphoreType.DMA,
            pltpu.SemaphoreType.DMA((9,)),
        ],
        compiler_params=pltpu.CompilerParams(collective_id=0, has_side_effects=True),
        name="window",
    )(tokens, queries, gains, key_weight, value_weight, lengths)


def solution(mesh):
    return jax.shard_map(
        body,
        mesh=mesh,
        in_specs=(
            P("section", None, "fsdp", None),
            P("section", None, "fsdp", None),
            P("section", None),
            P("section", "fsdp", None),
            P("section", "fsdp", None),
            P(),
        ),
        out_specs=P("section", None, "fsdp", None),
        check_vma=False,
    )
```

```python
import functools

import jax
import jax.numpy as jnp
from jax import lax
from jax.experimental import pallas as pl
from jax.experimental.pallas import tpu as pltpu
from jax.sharding import PartitionSpec as P

HEAD = 128
GROUPS = 4
FAN = 8
MICRO = 2
TOK = 128
ROWS = 256
BLOCKS = 16
HALF = ROWS * BLOCKS
WIDE = 2 * HEAD
DOCS = 64
XCUT = 4
MESH = pl.DeviceIdType.MESH

EVEN = (
    (((0, 0),), ((0, 1),), ((0, 2),), ((0, 3),), ((1, 2),)),
    (((0, 0),), ((0, -1),), ((0, -2),), ((1, 0),), ((1, -1),)),
    (((0, 0),), ((0, 1),), ((0, 2),), ((0, -3),), ((0, 4),)),
)
BACK = (
    (((0, 0),), ((0, 1),), ((0, 2),), ((1, 2),), ()),
    (((0, 0),), ((0, -1),), ((0, -2), (1, 0)), ((0, -3),), ((1, -1),)),
    (((0, 0),), ((0, 1),), ((0, 2),), ((0, -3),), ((0, -4),)),
)
SIDE = (
    (((0, 0),), ((0, 1),), ((0, 2),), ((0, 3),), ((1, 3, 1), (1, -3, 1))),
    (((0, 0),), ((0, -1),), ((0, -2),), ((1, 0),), ((1, -1, 0),)),
    (((0, 0),), ((0, 1),), ((0, 2),), ((0, 3), (0, -3)), ((0, 4, 0),)),
)
PATTERN = (EVEN, EVEN, BACK, SIDE)
MOVES = ((0, 1), (0, -1), (1, 0))
SENDS = [[[(p, item) for p, items in enumerate(link) for item in items] for link in pattern] for pattern in PATTERN]
ARRIVALS = [
    {
        ((r + MOVES[k][0]) % 2, d + MOVES[k][1], *part): (k, i)
        for k, link in enumerate(links)
        for i, (_, (r, d, *part)) in enumerate(link)
    }
    for links in SENDS
]
JOINT = {(g, p) for g in range(GROUPS) for p in range(5 if g < 2 else 2)}
PLACE, _semaphores = {}, {}
for _g, _links in enumerate(SENDS):
    for _k, _link in enumerate(_links):
        for _i, (_p, _) in enumerate(_link):
            _name = (_g, _p) if (_g, _p) in JOINT else (_g, _k, _i)
            PLACE[_g, _k, _i] = _semaphores.setdefault(_name, len(_semaphores))
LATE = ((), (), ((0, -4), (1, -2), (1, -4)), ((1, -1), (1, -3), (1, -2), (1, 4)))


def kernel(
    tok, queries, gains, key_w, value_w, lengths, out,
    wbuf, xown, xoth, xprt, xn, gown, qbuf, lens, inv_own, inv_send, inv_recv,
    bias, acc, p_own, p_send, p_recv, kv, passing,
    w_send, w_recv, x_send, x_recv, i_send, i_recv, p_ssem, p_rsem, h_send, h_recv, r_send, r_recv, b_send, local,
):
    me = lax.axis_index("fsdp")
    y, z = me // 8, me % 8
    half, row = y // 2, y % 2
    second = lax.axis_index("section") % 2 == 1
    z_next, z_prev = y * 8 + (z + 1) % 8, y * 8 + (z + 7) % 8
    mate = (y + 1 - 2 * row) * 8 + z
    partner = (3 - y) * 8 + z
    below = jnp.minimum(me + 8, 31)
    after, before = (me + 1) % 32, (me + 31) % 32

    def block_at(r, d):
        source_row = row if r == 0 else 1 - row
        source_z = (z - d + 8) % 8
        return pl.ds(pl.multiple_of((source_row * 8 + source_z) * ROWS, ROWS), ROWS)

    own_rows = block_at(0, 0)
    own_cols = pl.multiple_of(half * HALF, HALF)
    other_cols = pl.multiple_of((1 - half) * HALF, HALF)

    loads = []
    w_loads = []
    for g in range(GROUPS):
        cols = pl.ds(g * HEAD, HEAD)
        w_loads.append((
            pltpu.make_async_copy(key_w.at[0, :, cols], wbuf.at[g, own_rows, pl.ds(0, HEAD)], local.at[g]),
            pltpu.make_async_copy(value_w.at[0, :, cols], wbuf.at[g, own_rows, pl.ds(HEAD, HEAD)], local.at[g]),
        ))
    for pair in w_loads:
        for c in pair:
            c.start()
    x_other = pltpu.make_async_copy(tok.at[0, :, :, pl.ds(other_cols, HALF)], xoth, local.at[4])
    x_mine = pltpu.make_async_copy(tok.at[0, :, :, pl.ds(own_cols, HALF)], xown, local.at[5])
    g_load = pltpu.make_async_copy(gains.at[:, pl.ds(own_cols, HALF)], gown, local.at[6])
    l_load = pltpu.make_async_copy(lengths, lens, local.at[7])
    q_load = pltpu.make_async_copy(queries.at[0], qbuf, local.at[8])
    for c in (x_other, x_mine, g_load, l_load, q_load):
        c.start()

    @pl.when(me == 0)
    def _():
        for g in range(GROUPS):
            kv[g, :, 0:TOK, :] = jnp.zeros((MICRO, TOK, WIDE), jnp.bfloat16)

    barrier = pltpu.get_barrier_semaphore()
    for device in (z_next, z_prev, mate, partner, after, before):
        pl.semaphore_signal(barrier, inc=1, device_id={"fsdp": device}, device_id_type=MESH)
    def barrier_wait():
        pl.semaphore_wait(barrier, 6)

    barrier_wait()

    targets = (z_next, z_prev, mate)
    here = [{(0, 0)} for _ in range(GROUPS)]

    def w_ref(g, r, d, *part):
        rows = block_at(r, d)
        return wbuf.at[g, rows, pl.ds(part[0] * HEAD, HEAD)] if part else wbuf.at[g, rows]

    def w_copy(g, k, i, ref):
        return pltpu.make_async_remote_copy(
            src_ref=ref,
            dst_ref=ref,
            send_sem=w_send,
            recv_sem=w_recv.at[PLACE[g, k, i]],
            device_id={"fsdp": targets[k]},
            device_id_type=MESH,
        )

    def w_need(g, item):
        if item in here[g]:
            return
        here[g].add(item)
        if item not in ARRIVALS[g]:
            for half in (0, 1):
                w_need(g, (*item, half))
            return
        k, i = ARRIVALS[g][item]
        p = SENDS[g][k][i][0]
        if (g, p) in JOINT:
            together = {it for it, (kk, ii) in ARRIVALS[g].items() if SENDS[g][kk][ii][0] == p}
            here[g].update(together)
            w_copy(g, k, i, wbuf.at[g, pl.ds(0, len(together) * ROWS)]).wait_recv()
        else:
            w_copy(g, k, i, w_ref(g, *item)).wait_recv()

    def w_step(g, p, links=(0, 1, 2), at=None):
        for k in links:
            for i, (position, item) in enumerate(SENDS[g][k]):
                if position == p and at in (None, item):
                    w_need(g, item[:2])
                    w_copy(g, k, i, w_ref(g, *item)).start()

    def w_late(g):
        return LATE[g]

    def w_early(g):
        return [(0, 0)] + [item for item in ARRIVALS[g] if item[:2] not in LATE[g]]

    def w_rest(g, items):
        for item in items:
            w_need(g, item)

    def w_loaded(g):
        both = wbuf.at[g, own_rows]
        pltpu.make_async_copy(both, both, local.at[g]).wait()

    def x_copy(j):
        width = HALF // XCUT
        return pltpu.make_async_remote_copy(
            src_ref=xoth.at[:, :, pl.ds(j * width, width)],
            dst_ref=xprt.at[:, :, pl.ds(j * width, width)],
            send_sem=x_send,
            recv_sem=x_recv.at[j],
            device_id={"fsdp": partner},
            device_id_type=MESH,
        )

    def inv_copy():
        return pltpu.make_async_remote_copy(
            src_ref=inv_send, dst_ref=inv_recv, send_sem=i_send, recv_sem=i_recv,
            device_id={"fsdp": partner}, device_id_type=MESH,
        )

    def pieces(g):
        return ((0, WIDE),) if g < 3 else ((0, HEAD), (HEAD, HEAD))

    def part_copy(g, m, c):
        first, width = pieces(g)[c]
        at = (g, pl.ds(m * TOK, TOK), pl.ds(first, width))
        return pltpu.make_async_remote_copy(
            src_ref=p_send.at[at], dst_ref=p_recv.at[at],
            send_sem=p_ssem, recv_sem=p_rsem.at[g + c, m],
            device_id={"fsdp": partner}, device_id_type=MESH,
        )

    def halo_to(g, m, device, into=None, slot=0, c=0):
        first, width = pieces(g)[c]
        return pltpu.make_async_remote_copy(
            src_ref=kv.at[g, m, pl.ds(TOK, TOK), pl.ds(first, width)],
            dst_ref=kv.at[g, m, pl.ds(0, TOK), pl.ds(first, width)] if into is None else into,
            send_sem=h_send,
            recv_sem=(h_recv.at[g + c, m] if into is None else r_recv.at[g + slot]),
            device_id={"fsdp": device}, device_id_type=MESH,
        )

    def pass_on(g, m, device):
        return pltpu.make_async_remote_copy(
            src_ref=passing.at[g], dst_ref=kv.at[g, m, pl.ds(0, TOK)],
            send_sem=r_send, recv_sem=h_recv.at[g, m],
            device_id={"fsdp": device}, device_id_type=MESH,
        )

    def halo_start(g, m, c):
        @pl.when(z < 7)
        def _():
            halo_to(g, m, z_next, c=c).start()

        if g < 2:
            @pl.when((z == 7) & (y < 3))
            def _():
                halo_to(g, m, z_next if m == 1 else below, passing.at[g]).start()
        else:
            @pl.when((z == 7) & ((y == 0) | (y == 2)))
            def _():
                halo_to(g, m, after, c=c).start()

            if g == 2:
                @pl.when((z == 7) & (y == 1) & second)
                def _():
                    halo_to(g, m, below, passing.at[2 + m], m).start()

    def halo_last():
        for groups, turn in (((2, 3), jnp.logical_not(second)), ((3,), second)):
            @pl.when((z == 7) & (y == 1) & turn)
            def _():
                for g in groups:
                    for m in range(MICRO):
                        for c in range(len(pieces(g))):
                            halo_to(g, m, after, c=c).start()

    def pass_round(m):
        return pltpu.make_async_remote_copy(
            src_ref=passing.at[2 + m], dst_ref=kv.at[2, m, pl.ds(0, TOK)],
            send_sem=b_send, recv_sem=h_recv.at[2, m],
            device_id={"fsdp": z_next}, device_id_type=MESH,
        )

    def relay_round():
        @pl.when((z == 7) & (y == 2) & second)
        def _():
            for m in range(MICRO):
                halo_to(2, m, z_next, passing.at[2 + m], m).wait_recv()
                pass_round(m).start()

    def relay_first(g):
        @pl.when((z == 0) & (y < 3))
        def _():
            halo_to(g, 1, z_next, passing.at[g]).wait_recv()
            pass_on(g, 1, below).start()

    def relay_last(g):
        @pl.when((z == 7) & (y > 0))
        def _():
            halo_to(g, 0, z_next, passing.at[g]).wait_recv()
            pass_on(g, 0, z_next).start()

    def eye(n):
        return lax.broadcasted_iota(jnp.int32, (n, n), 0) == lax.broadcasted_iota(jnp.int32, (n, n), 1)

    def window():
        return lax.broadcasted_iota(jnp.int32, (TOK, TOK), 1) <= lax.broadcasted_iota(jnp.int32, (TOK, TOK), 0)

    def squares():
        for m in range(MICRO):
            def add(j, total):
                at = pl.ds(pl.multiple_of(j * 512, 512), 512)
                for x in (xown, xoth):
                    v = x[m, :, at].astype(jnp.float32)
                    v = v * v
                    for i in range(4):
                        total = total + v[:, i * 128:(i + 1) * 128]
                return total
            total = lax.fori_loop(0, HALF // 512, add, jnp.zeros((TOK, 128), jnp.float32))
            mean = jnp.sum(total, axis=1, keepdims=True) * (1.0 / (2 * HALF))
            inverse = jnp.broadcast_to(lax.rsqrt(mean + 1e-05), (TOK, 128))
            inv_own[m] = inverse
            inv_send[m:m + 1, :] = jnp.sum(jnp.where(eye(TOK), inverse, 0.0), axis=0, keepdims=True)

    def normalise(x, base, m, inverse, start, width):
        def one(j, _):
            at = pl.ds(pl.multiple_of(start + j * 256, 256), 256)
            v = x[m, :, at].astype(jnp.float32)
            scaled = v * jnp.concatenate([inverse, inverse], axis=1)
            xn[pl.ds(base + m * TOK, TOK), at] = (scaled * gown[:, at].astype(jnp.float32)).astype(jnp.bfloat16)
            return 0
        lax.fori_loop(0, width // 256, one, 0)

    def normalise_own():
        for m in range(MICRO):
            normalise(xown, 0, m, inv_own[m], 0, HALF)

    def normalise_partner(j):
        for m in range(MICRO):
            line = jnp.broadcast_to(inv_recv[m:m + 1, :], (TOK, TOK))
            column = jnp.sum(jnp.where(eye(TOK), line, 0.0), axis=1, keepdims=True)
            normalise(xprt, 2 * TOK, m, jnp.broadcast_to(column, (TOK, 128)), j * (HALF // XCUT), HALF // XCUT)

    def masks():
        for m in range(MICRO):
            lane = lax.broadcasted_iota(jnp.int32, (DOCS, DOCS), 1)
            sub = lax.broadcasted_iota(jnp.int32, (DOCS, DOCS), 0)
            line = jnp.broadcast_to(lens[m:m + 1, :].astype(jnp.float32), (DOCS, DOCS))
            bound_column = jnp.sum(jnp.where(lane <= sub, line, 0.0), axis=1, keepdims=True)
            column = jnp.sum(jnp.where(lane == sub, line, 0.0), axis=1, keepdims=True)
            bound_line = jnp.sum(jnp.where(sub <= lane, column, 0.0), axis=0, keepdims=True)
            start = me * TOK
            key_pos = (lax.broadcasted_iota(jnp.int32, (DOCS, 2 * TOK), 1) + (start - TOK)).astype(jnp.float32)
            key_doc = jnp.sum(jnp.where(bound_column <= key_pos, 1.0, 0.0), axis=0, keepdims=True)
            query_pos = (lax.broadcasted_iota(jnp.int32, (TOK, DOCS), 0) + start).astype(jnp.float32)
            query_doc = jnp.sum(jnp.where(bound_line <= query_pos, 1.0, 0.0), axis=1, keepdims=True)
            kp = lax.broadcasted_iota(jnp.int32, (TOK, 2 * TOK), 1) + (start - TOK)
            qp = lax.broadcasted_iota(jnp.int32, (TOK, 2 * TOK), 0) + start
            allowed = (key_doc == query_doc) & (kp <= qp) & (kp >= 0)
            merged = jnp.where(window(), jnp.where(allowed[:, TOK:], 1.0, 0.0), jnp.where(allowed[:, :TOK], 1.0, 0.0))
            bias[m] = jnp.where(merged > 0.5, 0.0, -1e30)

    def dot_own(g):
        p_own[g] = jnp.dot(xn[0:2 * TOK, :], wbuf[g], preferred_element_type=jnp.float32)

    def dot_partner(g):
        p_send[g] = jnp.dot(
            xn[2 * TOK:4 * TOK, :], wbuf[g], preferred_element_type=jnp.float32
        ).astype(jnp.bfloat16)
        for m in range(MICRO):
            part_copy(g, m, 0).start()

    def add_blocks(total, g, items, first, count):
        for item in items:
            at = block_at(*item)
            total = total + jnp.dot(
                xn[first:first + count, at], wbuf[g, at, :], preferred_element_type=jnp.float32
            )
        return total

    def dot_early(g):
        for first in (0, 2 * TOK):
            acc[g - 2, first:first + 2 * TOK] = add_blocks(
                jnp.zeros((2 * TOK, WIDE), jnp.float32), g, w_early(g), first, 2 * TOK
            )

    def dot_late(g):
        for m in range(MICRO):
            first = (2 + m) * TOK
            p_send[g, m * TOK:(m + 1) * TOK] = add_blocks(
                acc[g - 2, first:first + TOK], g, w_late(g), first, TOK
            ).astype(jnp.bfloat16)
            for c in range(len(pieces(g))):
                part_copy(g, m, c).start()
        p_own[g] = add_blocks(acc[g - 2, 0:2 * TOK], g, w_late(g), 0, 2 * TOK)

    def part_wait(g, m, c=0):
        part_copy(g, m, c).wait_recv()

    def halo_wait(g, m, c=0):
        @pl.when(me > 0)
        def _():
            halo_to(g, m, z_next, c=c).wait_recv()

    def x_wait(j):
        x_copy(j).wait_recv()

    def inv_wait():
        inv_copy().wait_recv()

    def start_wait():
        for c in (x_mine, g_load, l_load, q_load):
            c.wait()

    def finish_kv(g, m):
        at = pl.ds(m * TOK, TOK)
        for c, (first, width) in enumerate(pieces(g)):
            if c > 0:
                part_wait(g, m, c)
            cols = pl.ds(first, width)
            kv[g, m, TOK:2 * TOK, cols] = (p_own[g, at, cols] + p_recv[g, at, cols].astype(jnp.float32)).astype(jnp.bfloat16)
            halo_start(g, m, c)

    def attend(g, m):
        factor = HEAD ** (-0.5) * 1.4426950408889634
        keys = kv[g, m, :, 0:HEAD]
        own = window()
        held = []
        for j in range(FAN):
            at = pl.ds((g * FAN + j) * HEAD, HEAD)
            s = lax.dot_general(
                qbuf[m, :, at], keys, (((1,), (1,)), ((), ())), preferred_element_type=jnp.float32
            )
            s = jnp.where(own, s[:, TOK:], s[:, :TOK]) + bias[m]
            e = jnp.exp2((s - jnp.max(s, axis=1, keepdims=True)) * factor)
            weights = jnp.concatenate([jnp.where(own, 0.0, e), jnp.where(own, e, 0.0)], axis=1)
            held.append(weights.astype(jnp.bfloat16))
        if len(pieces(g)) > 1:
            halo_wait(g, m, 1)
        values = jnp.concatenate([kv[g, m, :, HEAD:WIDE], jnp.ones((2 * TOK, HEAD), jnp.bfloat16)], axis=1)
        for j in range(FAN):
            at = pl.ds((g * FAN + j) * HEAD, HEAD)
            mixed = jnp.dot(held[j], values, preferred_element_type=jnp.float32)
            out[0, m, :, at] = (mixed[:, :HEAD] * (1.0 / mixed[:, HEAD:])).astype(jnp.bfloat16)

    for g in (0, 1, 2):
        w_loaded(g)
        w_step(g, 0)
        if g == 0:
            x_other.wait()
            x_copy(0).start()
    w_loaded(3)
    start_wait()
    squares()
    inv_copy().start()
    for j in range(1, XCUT):
        x_copy(j).start()
    w_step(0, 1)
    normalise_own()
    w_step(1, 1)
    masks()
    w_step(0, 2)
    w_step(1, 2)
    w_step(0, 3)
    inv_wait()
    x_wait(0)
    normalise_partner(0)
    w_step(1, 3)
    w_step(0, 4)
    w_step(1, 4)
    w_step(3, 0)
    x_wait(1)
    normalise_partner(1)
    w_step(2, 1)
    w_rest(0, ARRIVALS[0])
    dot_own(0)
    w_rest(1, ARRIVALS[1])
    dot_own(1)
    w_step(3, 1)
    w_step(2, 2)
    x_wait(2)
    normalise_partner(2)
    w_step(3, 2)
    w_step(2, 3)
    x_wait(3)
    normalise_partner(3)
    w_step(3, 3, (0, 2, 1), (0, 3))
    w_step(3, 3, (1,))
    dot_partner(0)
    dot_partner(1)
    w_step(3, 3, (2,), (0, -3))
    w_rest(2, w_early(2))
    dot_early(2)
    for m in range(MICRO):
        part_wait(0, m)
        finish_kv(0, m)
    w_step(2, 4)
    w_step(3, 4, (2,))
    w_step(3, 4, (0,), (1, 3, 1))
    w_rest(3, w_early(3))
    dot_early(3)
    w_step(3, 4, (1,))
    w_step(3, 4, (0,), (1, -3, 1))
    for m in range(MICRO):
        part_wait(1, m)
        finish_kv(1, m)
    relay_first(0)
    relay_last(0)
    w_rest(2, w_late(2))
    dot_late(2)
    edge = (z == 0) & (y > 0)

    @pl.when(jnp.logical_not(edge) & (z < 7))
    def _():
        for m in range(MICRO):
            halo_wait(0, m)
            attend(0, m)

    w_rest(3, w_late(3))
    dot_late(3)
    relay_first(1)
    relay_last(1)

    @pl.when(edge)
    def _():
        halo_wait(0, 0)
        attend(0, 0)

    for m in range(MICRO):
        part_wait(2, m)
        finish_kv(2, m)
    part_wait(3, 0)
    finish_kv(3, 0)

    @pl.when(edge)
    def _():
        halo_wait(0, 1)
        attend(0, 1)

    @pl.when(jnp.logical_not(edge))
    def _():
        halo_wait(1, 0)
        attend(1, 0)

    part_wait(3, 1)
    finish_kv(3, 1)
    @pl.when(z == 7)
    def _():
        for m in range(MICRO):
            halo_wait(0, m)
            attend(0, m)

    halo_last()

    halo_wait(1, 1)
    attend(1, 1)
    relay_round()

    @pl.when(edge)
    def _():
        halo_wait(1, 0)
        attend(1, 0)

    for g in (2, 3):
        for m in range(MICRO):
            halo_wait(g, m)
            attend(g, m)

    def tail_wait():
        sent = wbuf.at[:, pl.ds(0, HALF - ROWS)]
        pltpu.make_async_remote_copy(
            src_ref=sent, dst_ref=sent, send_sem=w_send, recv_sem=w_recv.at[0],
            device_id={"fsdp": mate}, device_id_type=MESH,
        ).wait_send()
        pltpu.make_async_remote_copy(
            src_ref=xoth, dst_ref=xprt, send_sem=x_send, recv_sem=x_recv.at[0],
            device_id={"fsdp": partner}, device_id_type=MESH,
        ).wait_send()
        inv_copy().wait_send()
        pltpu.make_async_remote_copy(
            src_ref=p_send, dst_ref=p_recv, send_sem=p_ssem, recv_sem=p_rsem.at[0, 0],
            device_id={"fsdp": partner}, device_id_type=MESH,
        ).wait_send()

        @pl.when(me < 31)
        def _():
            rows = kv.at[:, :, pl.ds(0, TOK)]
            pltpu.make_async_remote_copy(
                src_ref=rows, dst_ref=rows, send_sem=h_send, recv_sem=h_recv.at[0, 0],
                device_id={"fsdp": z_next}, device_id_type=MESH,
            ).wait_send()

        @pl.when(((z == 0) & (y < 3)) | ((z == 7) & (y > 0)))
        def _():
            pltpu.make_async_remote_copy(
                src_ref=passing.at[pl.ds(0, 2)], dst_ref=passing.at[pl.ds(0, 2)], send_sem=r_send, recv_sem=r_recv.at[0],
                device_id={"fsdp": z_next}, device_id_type=MESH,
            ).wait_send()

        @pl.when((z == 7) & (y == 2) & second)
        def _():
            both = passing.at[pl.ds(2, 2)]
            pltpu.make_async_remote_copy(
                src_ref=both, dst_ref=both, send_sem=b_send, recv_sem=r_recv.at[2],
                device_id={"fsdp": z_next}, device_id_type=MESH,
            ).wait_send()

    tail_wait()


def body(tokens, queries, gains, key_weight, value_weight, lengths):
    bf16, f32 = jnp.bfloat16, jnp.float32
    return pl.pallas_call(
        kernel,
        out_shape=pltpu.VMEM(queries.shape, bf16),
        in_specs=[pl.BlockSpec(memory_space=pl.ANY)] * 6,
        out_specs=pl.BlockSpec(memory_space=pltpu.VMEM),
        scratch_shapes=[
            pltpu.VMEM((GROUPS, HALF, WIDE), bf16),
            pltpu.VMEM((MICRO, TOK, HALF), bf16),
            pltpu.VMEM((MICRO, TOK, HALF), bf16),
            pltpu.VMEM((MICRO, TOK, HALF), bf16),
            pltpu.VMEM((4 * TOK, HALF), bf16),
            pltpu.VMEM((1, HALF), bf16),
            pltpu.VMEM((MICRO, TOK, GROUPS * FAN * HEAD), bf16),
            pltpu.VMEM((MICRO, DOCS), jnp.int32),
            pltpu.VMEM((MICRO, TOK, 128), f32),
            pltpu.VMEM((8, 128), f32),
            pltpu.VMEM((8, 128), f32),
            pltpu.VMEM((MICRO, TOK, TOK), f32),
            pltpu.VMEM((2, 4 * TOK, WIDE), f32),
            pltpu.VMEM((GROUPS, 2 * TOK, WIDE), f32),
            pltpu.VMEM((GROUPS, 2 * TOK, WIDE), bf16),
            pltpu.VMEM((GROUPS, 2 * TOK, WIDE), bf16),
            pltpu.VMEM((GROUPS, MICRO, 2 * TOK, WIDE), bf16),
            pltpu.VMEM((4, TOK, WIDE), bf16),
            pltpu.SemaphoreType.DMA,
            pltpu.SemaphoreType.DMA((len(_semaphores),)),
            pltpu.SemaphoreType.DMA,
            pltpu.SemaphoreType.DMA((XCUT,)),
            pltpu.SemaphoreType.DMA,
            pltpu.SemaphoreType.DMA,
            pltpu.SemaphoreType.DMA,
            pltpu.SemaphoreType.DMA((GROUPS + 1, MICRO)),
            pltpu.SemaphoreType.DMA,
            pltpu.SemaphoreType.DMA((GROUPS + 1, MICRO)),
            pltpu.SemaphoreType.DMA,
            pltpu.SemaphoreType.DMA((4,)),
            pltpu.SemaphoreType.DMA,
            pltpu.SemaphoreType.DMA((9,)),
        ],
        compiler_params=pltpu.CompilerParams(collective_id=0, has_side_effects=True),
        name="window",
    )(tokens, queries, gains, key_weight, value_weight, lengths)


def solution(mesh):
    return jax.shard_map(
        body,
        mesh=mesh,
        in_specs=(
            P("section", None, "fsdp", None),
            P("section", None, "fsdp", None),
            P("section", None),
            P("section", "fsdp", None),
            P("section", "fsdp", None),
            P(),
        ),
        out_specs=P("section", None, "fsdp", None),
        check_vma=False,
    )
```

```python
import functools

import jax
import jax.numpy as jnp
from jax import lax
from jax.experimental import pallas as pl
from jax.experimental.pallas import tpu as pltpu
from jax.sharding import PartitionSpec as P

HEAD = 128
GROUPS = 4
FAN = 8
MICRO = 2
TOK = 128
ROWS = 256
BLOCKS = 16
HALF = ROWS * BLOCKS
WIDE = 2 * HEAD
DOCS = 64
XCUT = 4
MESH = pl.DeviceIdType.MESH

EVEN = (
    (((0, 0),), ((0, 1),), ((0, 2),), ((0, 3),), ((1, 2),)),
    (((0, 0),), ((0, -1),), ((0, -2),), ((1, 0),), ((1, -1),)),
    (((0, 0),), ((0, 1),), ((0, 2),), ((0, -3),), ((0, 4),)),
)
BACK = (
    (((0, 0),), ((0, 1),), ((0, 2),), ((1, 2),), ()),
    (((0, 0),), ((0, -1),), ((0, -2), (1, 0)), ((0, -3),), ((1, -1),)),
    (((0, 0),), ((0, 1),), ((0, 2),), ((0, -3),), ((0, -4),)),
)
SIDE = (
    (((0, 0),), ((0, 1),), ((0, 2),), ((0, 3),), ((1, 3, 1), (1, -3, 1))),
    (((0, 0),), ((0, -1),), ((0, -2),), ((1, 0),), ((1, -1, 0),)),
    (((0, 0),), ((0, 1),), ((0, 2),), ((0, 3), (0, -3)), ((0, 4, 0),)),
)
PATTERN = (EVEN, EVEN, BACK, SIDE)
MOVES = ((0, 1), (0, -1), (1, 0))
SENDS = [[[(p, item) for p, items in enumerate(link) for item in items] for link in pattern] for pattern in PATTERN]
ARRIVALS = [
    {
        ((r + MOVES[k][0]) % 2, d + MOVES[k][1], *part): (k, i)
        for k, link in enumerate(links)
        for i, (_, (r, d, *part)) in enumerate(link)
    }
    for links in SENDS
]
JOINT = {(g, p) for g in range(GROUPS) for p in range(5 if g < 2 else 2)}
PLACE, _semaphores = {}, {}
for _g, _links in enumerate(SENDS):
    for _k, _link in enumerate(_links):
        for _i, (_p, _) in enumerate(_link):
            _name = (_g, _p) if (_g, _p) in JOINT else (_g, _k, _i)
            PLACE[_g, _k, _i] = _semaphores.setdefault(_name, len(_semaphores))
LATE = ((), (), ((0, -4), (1, -2), (1, -4)), ((1, -1), (1, -3), (1, -2), (1, 4)))


def kernel(
    tok, queries, gains, key_w, value_w, lengths, out,
    wbuf, xown, xoth, xprt, xn, gown, qbuf, lens, inv_own, inv_send, inv_recv,
    bias, acc, p_own, p_send, p_recv, kv, passing,
    w_send, w_recv, x_send, x_recv, i_send, i_recv, p_ssem, p_rsem, h_send, h_recv, r_send, r_recv, b_send, local,
):
    me = lax.axis_index("fsdp")
    y, z = me // 8, me % 8
    half, row = y // 2, y % 2
    second = lax.axis_index("section") % 2 == 1
    z_next, z_prev = y * 8 + (z + 1) % 8, y * 8 + (z + 7) % 8
    mate = (y + 1 - 2 * row) * 8 + z
    partner = (3 - y) * 8 + z
    below = jnp.minimum(me + 8, 31)
    after, before = (me + 1) % 32, (me + 31) % 32

    def block_at(r, d):
        source_row = row if r == 0 else 1 - row
        source_z = (z - d + 8) % 8
        return pl.ds(pl.multiple_of((source_row * 8 + source_z) * ROWS, ROWS), ROWS)

    own_rows = block_at(0, 0)
    own_cols = pl.multiple_of(half * HALF, HALF)
    other_cols = pl.multiple_of((1 - half) * HALF, HALF)

    loads = []
    w_loads = []
    for g in range(GROUPS):
        cols = pl.ds(g * HEAD, HEAD)
        w_loads.append((
            pltpu.make_async_copy(key_w.at[0, :, cols], wbuf.at[g, own_rows, pl.ds(0, HEAD)], local.at[g]),
            pltpu.make_async_copy(value_w.at[0, :, cols], wbuf.at[g, own_rows, pl.ds(HEAD, HEAD)], local.at[g]),
        ))
    for pair in w_loads:
        for c in pair:
            c.start()
    x_other = pltpu.make_async_copy(tok.at[0, :, :, pl.ds(other_cols, HALF)], xoth, local.at[4])
    x_mine = pltpu.make_async_copy(tok.at[0, :, :, pl.ds(own_cols, HALF)], xown, local.at[5])
    g_load = pltpu.make_async_copy(gains.at[:, pl.ds(own_cols, HALF)], gown, local.at[6])
    l_load = pltpu.make_async_copy(lengths, lens, local.at[7])
    q_load = pltpu.make_async_copy(queries.at[0], qbuf, local.at[8])
    for c in (x_other, x_mine, g_load, l_load, q_load):
        c.start()

    @pl.when(me == 0)
    def _():
        for g in range(GROUPS):
            kv[g, :, 0:TOK, :] = jnp.zeros((MICRO, TOK, WIDE), jnp.bfloat16)

    barrier = pltpu.get_barrier_semaphore()
    for device in (z_next, z_prev, mate, partner, after, before):
        pl.semaphore_signal(barrier, inc=1, device_id={"fsdp": device}, device_id_type=MESH)
    def barrier_wait():
        pl.semaphore_wait(barrier, 6)

    barrier_wait()

    targets = (z_next, z_prev, mate)
    here = [{(0, 0)} for _ in range(GROUPS)]

    def w_ref(g, r, d, *part):
        rows = block_at(r, d)
        return wbuf.at[g, rows, pl.ds(part[0] * HEAD, HEAD)] if part else wbuf.at[g, rows]

    def w_copy(g, k, i, ref):
        return pltpu.make_async_remote_copy(
            src_ref=ref,
            dst_ref=ref,
            send_sem=w_send,
            recv_sem=w_recv.at[PLACE[g, k, i]],
            device_id={"fsdp": targets[k]},
            device_id_type=MESH,
        )

    def w_need(g, item):
        if item in here[g]:
            return
        here[g].add(item)
        if item not in ARRIVALS[g]:
            for half in (0, 1):
                w_need(g, (*item, half))
            return
        k, i = ARRIVALS[g][item]
        p = SENDS[g][k][i][0]
        if (g, p) in JOINT:
            together = {it for it, (kk, ii) in ARRIVALS[g].items() if SENDS[g][kk][ii][0] == p}
            here[g].update(together)
            w_copy(g, k, i, wbuf.at[g, pl.ds(0, len(together) * ROWS)]).wait_recv()
        else:
            w_copy(g, k, i, w_ref(g, *item)).wait_recv()

    def w_step(g, p, links=(0, 1, 2), at=None):
        for k in links:
            for i, (position, item) in enumerate(SENDS[g][k]):
                if position == p and at in (None, item):
                    w_need(g, item[:2])
                    w_copy(g, k, i, w_ref(g, *item)).start()

    def w_late(g):
        return LATE[g]

    def w_early(g):
        return [(0, 0)] + [item for item in ARRIVALS[g] if item[:2] not in LATE[g]]

    def w_rest(g, items):
        for item in items:
            w_need(g, item)

    def w_loaded(g):
        both = wbuf.at[g, own_rows]
        pltpu.make_async_copy(both, both, local.at[g]).wait()

    def x_copy(j):
        width = HALF // XCUT
        return pltpu.make_async_remote_copy(
            src_ref=xoth.at[:, :, pl.ds(j * width, width)],
            dst_ref=xprt.at[:, :, pl.ds(j * width, width)],
            send_sem=x_send,
            recv_sem=x_recv.at[j],
            device_id={"fsdp": partner},
            device_id_type=MESH,
        )

    def inv_copy():
        return pltpu.make_async_remote_copy(
            src_ref=inv_send, dst_ref=inv_recv, send_sem=i_send, recv_sem=i_recv,
            device_id={"fsdp": partner}, device_id_type=MESH,
        )

    def pieces(g):
        return ((0, WIDE),) if g < 3 else ((0, HEAD), (HEAD, HEAD))

    def part_copy(g, m, c):
        first, width = pieces(g)[c]
        at = (g, pl.ds(m * TOK, TOK), pl.ds(first, width))
        return pltpu.make_async_remote_copy(
            src_ref=p_send.at[at], dst_ref=p_recv.at[at],
            send_sem=p_ssem, recv_sem=p_rsem.at[g + c, m],
            device_id={"fsdp": partner}, device_id_type=MESH,
        )

    def halo_to(g, m, device, into=None, c=0):
        first, width = pieces(g)[c]
        return pltpu.make_async_remote_copy(
            src_ref=kv.at[g, m, pl.ds(TOK, TOK), pl.ds(first, width)],
            dst_ref=kv.at[g, m, pl.ds(0, TOK), pl.ds(first, width)] if into is None else into,
            send_sem=h_send,
            recv_sem=(h_recv.at[g + c, m] if into is None else r_recv.at[g]),
            device_id={"fsdp": device}, device_id_type=MESH,
        )

    def pass_on(g, m, device):
        return pltpu.make_async_remote_copy(
            src_ref=passing.at[g], dst_ref=kv.at[g, m, pl.ds(0, TOK)],
            send_sem=r_send, recv_sem=h_recv.at[g, m],
            device_id={"fsdp": device}, device_id_type=MESH,
        )

    def halo_start(g, m, c):
        @pl.when(z < 7)
        def _():
            halo_to(g, m, z_next, c=c).start()

        if g < 2:
            @pl.when((z == 7) & (y < 3))
            def _():
                halo_to(g, m, z_next if m == 1 else below, passing.at[g]).start()
        else:
            @pl.when((z == 7) & ((y == 0) | (y == 2)))
            def _():
                halo_to(g, m, after, c=c).start()

            if (g, m) == (2, 0):
                @pl.when((z == 7) & (y == 1) & second)
                def _():
                    halo_to(g, m, below, passing.at[2]).start()

    def halo_last():
        for first, turn in ((0, jnp.logical_not(second)), (1, second)):
            @pl.when((z == 7) & (y == 1) & turn)
            def _():
                for g, m in ((2, 0), (2, 1), (3, 0), (3, 1))[first:]:
                    for c in range(len(pieces(g))):
                        halo_to(g, m, after, c=c).start()

    def pass_round():
        return pltpu.make_async_remote_copy(
            src_ref=passing.at[2], dst_ref=kv.at[2, 0, pl.ds(0, TOK)],
            send_sem=b_send, recv_sem=h_recv.at[2, 0],
            device_id={"fsdp": z_next}, device_id_type=MESH,
        )

    def relay_round():
        @pl.when((z == 7) & (y == 2) & second)
        def _():
            halo_to(2, 0, z_next, passing.at[2]).wait_recv()
            pass_round().start()

    def relay_first(g):
        @pl.when((z == 0) & (y < 3))
        def _():
            halo_to(g, 1, z_next, passing.at[g]).wait_recv()
            pass_on(g, 1, below).start()

    def relay_last(g):
        @pl.when((z == 7) & (y > 0))
        def _():
            halo_to(g, 0, z_next, passing.at[g]).wait_recv()
            pass_on(g, 0, z_next).start()

    def eye(n):
        return lax.broadcasted_iota(jnp.int32, (n, n), 0) == lax.broadcasted_iota(jnp.int32, (n, n), 1)

    def window():
        return lax.broadcasted_iota(jnp.int32, (TOK, TOK), 1) <= lax.broadcasted_iota(jnp.int32, (TOK, TOK), 0)

    def squares():
        for m in range(MICRO):
            def add(j, total):
                at = pl.ds(pl.multiple_of(j * 512, 512), 512)
                for x in (xown, xoth):
                    v = x[m, :, at].astype(jnp.float32)
                    v = v * v
                    for i in range(4):
                        total = total + v[:, i * 128:(i + 1) * 128]
                return total
            total = lax.fori_loop(0, HALF // 512, add, jnp.zeros((TOK, 128), jnp.float32))
            mean = jnp.sum(total, axis=1, keepdims=True) * (1.0 / (2 * HALF))
            inverse = jnp.broadcast_to(lax.rsqrt(mean + 1e-05), (TOK, 128))
            inv_own[m] = inverse
            inv_send[m:m + 1, :] = jnp.sum(jnp.where(eye(TOK), inverse, 0.0), axis=0, keepdims=True)

    def normalise(x, base, m, inverse, start, width):
        def one(j, _):
            at = pl.ds(pl.multiple_of(start + j * 256, 256), 256)
            v = x[m, :, at].astype(jnp.float32)
            scaled = v * jnp.concatenate([inverse, inverse], axis=1)
            xn[pl.ds(base + m * TOK, TOK), at] = (scaled * gown[:, at].astype(jnp.float32)).astype(jnp.bfloat16)
            return 0
        lax.fori_loop(0, width // 256, one, 0)

    def normalise_own():
        for m in range(MICRO):
            normalise(xown, 0, m, inv_own[m], 0, HALF)

    def normalise_partner(j):
        for m in range(MICRO):
            line = jnp.broadcast_to(inv_recv[m:m + 1, :], (TOK, TOK))
            column = jnp.sum(jnp.where(eye(TOK), line, 0.0), axis=1, keepdims=True)
            normalise(xprt, 2 * TOK, m, jnp.broadcast_to(column, (TOK, 128)), j * (HALF // XCUT), HALF // XCUT)

    def masks():
        for m in range(MICRO):
            lane = lax.broadcasted_iota(jnp.int32, (DOCS, DOCS), 1)
            sub = lax.broadcasted_iota(jnp.int32, (DOCS, DOCS), 0)
            line = jnp.broadcast_to(lens[m:m + 1, :].astype(jnp.float32), (DOCS, DOCS))
            bound_column = jnp.sum(jnp.where(lane <= sub, line, 0.0), axis=1, keepdims=True)
            column = jnp.sum(jnp.where(lane == sub, line, 0.0), axis=1, keepdims=True)
            bound_line = jnp.sum(jnp.where(sub <= lane, column, 0.0), axis=0, keepdims=True)
            start = me * TOK
            key_pos = (lax.broadcasted_iota(jnp.int32, (DOCS, 2 * TOK), 1) + (start - TOK)).astype(jnp.float32)
            key_doc = jnp.sum(jnp.where(bound_column <= key_pos, 1.0, 0.0), axis=0, keepdims=True)
            query_pos = (lax.broadcasted_iota(jnp.int32, (TOK, DOCS), 0) + start).astype(jnp.float32)
            query_doc = jnp.sum(jnp.where(bound_line <= query_pos, 1.0, 0.0), axis=1, keepdims=True)
            kp = lax.broadcasted_iota(jnp.int32, (TOK, 2 * TOK), 1) + (start - TOK)
            qp = lax.broadcasted_iota(jnp.int32, (TOK, 2 * TOK), 0) + start
            allowed = (key_doc == query_doc) & (kp <= qp) & (kp >= 0)
            merged = jnp.where(window(), jnp.where(allowed[:, TOK:], 1.0, 0.0), jnp.where(allowed[:, :TOK], 1.0, 0.0))
            bias[m] = jnp.where(merged > 0.5, 0.0, -1e30)

    def dot_own(g):
        p_own[g] = jnp.dot(xn[0:2 * TOK, :], wbuf[g], preferred_element_type=jnp.float32)

    def dot_partner(g):
        p_send[g] = jnp.dot(
            xn[2 * TOK:4 * TOK, :], wbuf[g], preferred_element_type=jnp.float32
        ).astype(jnp.bfloat16)
        for m in range(MICRO):
            part_copy(g, m, 0).start()

    def add_blocks(total, g, items, first, count):
        for item in items:
            at = block_at(*item)
            total = total + jnp.dot(
                xn[first:first + count, at], wbuf[g, at, :], preferred_element_type=jnp.float32
            )
        return total

    def dot_early(g):
        for first in (0, 2 * TOK):
            acc[g - 2, first:first + 2 * TOK] = add_blocks(
                jnp.zeros((2 * TOK, WIDE), jnp.float32), g, w_early(g), first, 2 * TOK
            )

    def dot_late(g):
        for m in range(MICRO):
            first = (2 + m) * TOK
            p_send[g, m * TOK:(m + 1) * TOK] = add_blocks(
                acc[g - 2, first:first + TOK], g, w_late(g), first, TOK
            ).astype(jnp.bfloat16)
            for c in range(len(pieces(g))):
                part_copy(g, m, c).start()
        p_own[g] = add_blocks(acc[g - 2, 0:2 * TOK], g, w_late(g), 0, 2 * TOK)

    def part_wait(g, m, c=0):
        part_copy(g, m, c).wait_recv()

    def halo_wait(g, m, c=0):
        @pl.when(me > 0)
        def _():
            halo_to(g, m, z_next, c=c).wait_recv()

    def x_wait(j):
        x_copy(j).wait_recv()

    def inv_wait():
        inv_copy().wait_recv()

    def start_wait():
        for c in (x_mine, g_load, l_load, q_load):
            c.wait()

    def finish_kv(g, m):
        at = pl.ds(m * TOK, TOK)
        for c, (first, width) in enumerate(pieces(g)):
            if c > 0:
                part_wait(g, m, c)
            cols = pl.ds(first, width)
            kv[g, m, TOK:2 * TOK, cols] = (p_own[g, at, cols] + p_recv[g, at, cols].astype(jnp.float32)).astype(jnp.bfloat16)
            halo_start(g, m, c)

    def attend(g, m):
        factor = HEAD ** (-0.5) * 1.4426950408889634
        keys = kv[g, m, :, 0:HEAD]
        own = window()
        held = []
        for j in range(FAN):
            at = pl.ds((g * FAN + j) * HEAD, HEAD)
            s = lax.dot_general(
                qbuf[m, :, at], keys, (((1,), (1,)), ((), ())), preferred_element_type=jnp.float32
            )
            s = jnp.where(own, s[:, TOK:], s[:, :TOK]) + bias[m]
            e = jnp.exp2((s - jnp.max(s, axis=1, keepdims=True)) * factor)
            weights = jnp.concatenate([jnp.where(own, 0.0, e), jnp.where(own, e, 0.0)], axis=1)
            held.append(weights.astype(jnp.bfloat16))
        if len(pieces(g)) > 1:
            halo_wait(g, m, 1)
        values = jnp.concatenate([kv[g, m, :, HEAD:WIDE], jnp.ones((2 * TOK, HEAD), jnp.bfloat16)], axis=1)
        for j in range(FAN):
            at = pl.ds((g * FAN + j) * HEAD, HEAD)
            mixed = jnp.dot(held[j], values, preferred_element_type=jnp.float32)
            out[0, m, :, at] = (mixed[:, :HEAD] * (1.0 / mixed[:, HEAD:])).astype(jnp.bfloat16)

    for g in (0, 1, 2):
        w_loaded(g)
        w_step(g, 0)
        if g == 0:
            x_other.wait()
            x_copy(0).start()
    w_loaded(3)
    start_wait()
    squares()
    inv_copy().start()
    for j in range(1, XCUT):
        x_copy(j).start()
    w_step(0, 1)
    normalise_own()
    w_step(1, 1)
    masks()
    w_step(0, 2)
    w_step(1, 2)
    w_step(0, 3)
    inv_wait()
    x_wait(0)
    normalise_partner(0)
    w_step(1, 3)
    w_step(0, 4)
    w_step(1, 4)
    w_step(3, 0)
    x_wait(1)
    normalise_partner(1)
    w_step(2, 1)
    w_rest(0, ARRIVALS[0])
    dot_own(0)
    w_rest(1, ARRIVALS[1])
    dot_own(1)
    w_step(3, 1)
    w_step(2, 2)
    x_wait(2)
    normalise_partner(2)
    w_step(3, 2)
    w_step(2, 3)
    x_wait(3)
    normalise_partner(3)
    w_step(3, 3, (0, 2, 1), (0, 3))
    w_step(3, 3, (1,))
    dot_partner(0)
    dot_partner(1)
    w_step(3, 3, (2,), (0, -3))
    w_rest(2, w_early(2))
    dot_early(2)
    for m in range(MICRO):
        part_wait(0, m)
        finish_kv(0, m)
    w_step(2, 4)
    w_step(3, 4, (2,))
    w_step(3, 4, (0,), (1, 3, 1))
    w_rest(3, w_early(3))
    dot_early(3)
    w_step(3, 4, (1,))
    w_step(3, 4, (0,), (1, -3, 1))
    for m in range(MICRO):
        part_wait(1, m)
        finish_kv(1, m)
    relay_first(0)
    relay_last(0)
    w_rest(2, w_late(2))
    dot_late(2)
    edge = (z == 0) & (y > 0)

    @pl.when(jnp.logical_not(edge) & (z < 7))
    def _():
        for m in range(MICRO):
            halo_wait(0, m)
            attend(0, m)

    w_rest(3, w_late(3))
    dot_late(3)
    relay_first(1)
    relay_last(1)

    @pl.when(edge)
    def _():
        halo_wait(0, 0)
        attend(0, 0)

    for m in range(MICRO):
        part_wait(2, m)
        finish_kv(2, m)
    part_wait(3, 0)
    finish_kv(3, 0)

    @pl.when(edge)
    def _():
        halo_wait(0, 1)
        attend(0, 1)

    @pl.when(jnp.logical_not(edge))
    def _():
        halo_wait(1, 0)
        attend(1, 0)

    part_wait(3, 1)
    finish_kv(3, 1)
    @pl.when(z == 7)
    def _():
        halo_wait(0, 0)
        attend(0, 0)

    halo_last()

    @pl.when(z == 7)
    def _():
        halo_wait(0, 1)
        attend(0, 1)


    halo_wait(1, 1)
    attend(1, 1)
    relay_round()

    @pl.when(edge)
    def _():
        halo_wait(1, 0)
        attend(1, 0)

    for g in (2, 3):
        for m in range(MICRO):
            halo_wait(g, m)
            attend(g, m)

    def tail_wait():
        sent = wbuf.at[:, pl.ds(0, HALF - ROWS)]
        pltpu.make_async_remote_copy(
            src_ref=sent, dst_ref=sent, send_sem=w_send, recv_sem=w_recv.at[0],
            device_id={"fsdp": mate}, device_id_type=MESH,
        ).wait_send()
        pltpu.make_async_remote_copy(
            src_ref=xoth, dst_ref=xprt, send_sem=x_send, recv_sem=x_recv.at[0],
            device_id={"fsdp": partner}, device_id_type=MESH,
        ).wait_send()
        inv_copy().wait_send()
        pltpu.make_async_remote_copy(
            src_ref=p_send, dst_ref=p_recv, send_sem=p_ssem, recv_sem=p_rsem.at[0, 0],
            device_id={"fsdp": partner}, device_id_type=MESH,
        ).wait_send()

        @pl.when(me < 31)
        def _():
            rows = kv.at[:, :, pl.ds(0, TOK)]
            pltpu.make_async_remote_copy(
                src_ref=rows, dst_ref=rows, send_sem=h_send, recv_sem=h_recv.at[0, 0],
                device_id={"fsdp": z_next}, device_id_type=MESH,
            ).wait_send()

        @pl.when(((z == 0) & (y < 3)) | ((z == 7) & (y > 0)))
        def _():
            pltpu.make_async_remote_copy(
                src_ref=passing.at[pl.ds(0, 2)], dst_ref=passing.at[pl.ds(0, 2)], send_sem=r_send, recv_sem=r_recv.at[0],
                device_id={"fsdp": z_next}, device_id_type=MESH,
            ).wait_send()

        @pl.when((z == 7) & (y == 2) & second)
        def _():
            pass_round().wait_send()

    tail_wait()


def body(tokens, queries, gains, key_weight, value_weight, lengths):
    bf16, f32 = jnp.bfloat16, jnp.float32
    return pl.pallas_call(
        kernel,
        out_shape=pltpu.VMEM(queries.shape, bf16),
        in_specs=[pl.BlockSpec(memory_space=pl.ANY)] * 6,
        out_specs=pl.BlockSpec(memory_space=pltpu.VMEM),
        scratch_shapes=[
            pltpu.VMEM((GROUPS, HALF, WIDE), bf16),
            pltpu.VMEM((MICRO, TOK, HALF), bf16),
            pltpu.VMEM((MICRO, TOK, HALF), bf16),
            pltpu.VMEM((MICRO, TOK, HALF), bf16),
            pltpu.VMEM((4 * TOK, HALF), bf16),
            pltpu.VMEM((1, HALF), bf16),
            pltpu.VMEM((MICRO, TOK, GROUPS * FAN * HEAD), bf16),
            pltpu.VMEM((MICRO, DOCS), jnp.int32),
            pltpu.VMEM((MICRO, TOK, 128), f32),
            pltpu.VMEM((8, 128), f32),
            pltpu.VMEM((8, 128), f32),
            pltpu.VMEM((MICRO, TOK, TOK), f32),
            pltpu.VMEM((2, 4 * TOK, WIDE), f32),
            pltpu.VMEM((GROUPS, 2 * TOK, WIDE), f32),
            pltpu.VMEM((GROUPS, 2 * TOK, WIDE), bf16),
            pltpu.VMEM((GROUPS, 2 * TOK, WIDE), bf16),
            pltpu.VMEM((GROUPS, MICRO, 2 * TOK, WIDE), bf16),
            pltpu.VMEM((3, TOK, WIDE), bf16),
            pltpu.SemaphoreType.DMA,
            pltpu.SemaphoreType.DMA((len(_semaphores),)),
            pltpu.SemaphoreType.DMA,
            pltpu.SemaphoreType.DMA((XCUT,)),
            pltpu.SemaphoreType.DMA,
            pltpu.SemaphoreType.DMA,
            pltpu.SemaphoreType.DMA,
            pltpu.SemaphoreType.DMA((GROUPS + 1, MICRO)),
            pltpu.SemaphoreType.DMA,
            pltpu.SemaphoreType.DMA((GROUPS + 1, MICRO)),
            pltpu.SemaphoreType.DMA,
            pltpu.SemaphoreType.DMA((3,)),
            pltpu.SemaphoreType.DMA,
            pltpu.SemaphoreType.DMA((9,)),
        ],
        compiler_params=pltpu.CompilerParams(collective_id=0, has_side_effects=True),
        name="window",
    )(tokens, queries, gains, key_weight, value_weight, lengths)


def solution(mesh):
    return jax.shard_map(
        body,
        mesh=mesh,
        in_specs=(
            P("section", None, "fsdp", None),
            P("section", None, "fsdp", None),
            P("section", None),
            P("section", "fsdp", None),
            P("section", "fsdp", None),
            P(),
        ),
        out_specs=P("section", None, "fsdp", None),
        check_vma=False,
    )
```
